32 devices in a mesh: slab: 4 (over y, core), patch: 8 (over z, x).
Axes of the slice: x: 2, y: 2, z: 4, core: 2. Of those that a mesh axis runs over, the one named last changes fastest.
Arguments:
- coarse: float32 [5, 64, 128, 128], P(None, 'slab', 'patch'), may hold values from -1.2 to 7.7, as said below
- fine: float32 [5, 128, 32, 1024], P(None, ('slab', 'patch')), may hold values from -1.2 to 7.7, as said below
- columns: int32 [32, 2], replicated, may hold values from 0 to 5, as said below
- patch_ids: int32 [4, 32], P('slab'), may hold values from 0 to 31, each once within a row
Outputs:
- coarse_out: float32 [5, 64, 128, 128], P(None, 'slab', 'patch')
- fine_out: float32 [5, 128, 32, 1024], P(None, ('slab', 'patch'))
The draws below stay inside these ranges and needn't reach their ends.
Inputs may be any that keep to these rules, and one draw needn't show every extreme that they name: `coarse`: conserved variables of states with density and pressure between 0.5 and 2 and velocity components between -0.6 and 1.4. `fine`: conserved variables of states with density and pressure between 0.5 and 2 and velocity components between -0.6 and 1.4. `columns`: 32 distinct pairs (gy, gz) with gy below 6 and gz below 6. `patch_ids`: each row is a permutation of the 32 patch numbers of a slab.
All inputs are finite; a program needn't handle non-finite values.
Results may differ from the reference program's by a relative error of at most 0.00005.
Values sent between devices are 32-bit elements; how exact they have to be, the bound alone decides.
No kernel may reach another device: no remote copies, remote signals or barrier semaphores. Data moves between devices by JAX's collectives and lax.ppermute only.
A program may use at most 320 MiB of HBM per device.

```python
import math
import jax
import jax.numpy as jnp
from jax import lax

P_SIZE = 32
LX = 1
GY = 6
GZ = 6
PYZ = 32
H = 16
SLOTS = 32
PATCHES = 128
NXC = 64
NZC = 128
NYC = 128
N_SLAB = 4


def conserved(key, extents):
    keys = jax.random.split(key, 5)
    density = jnp.exp(jax.random.uniform(keys[0], extents, minval=math.log(0.5), maxval=math.log(2.0)))
    pressure = jnp.exp(jax.random.uniform(keys[1], extents, minval=math.log(0.5), maxval=math.log(2.0)))
    velocity_x = jax.random.uniform(keys[2], extents, minval=-0.6, maxval=0.6)
    velocity_y = jax.random.uniform(keys[3], extents, minval=-0.6, maxval=0.6)
    velocity_z = jax.random.uniform(keys[4], extents, minval=-0.6, maxval=0.6)
    energy = pressure / 0.4 + 0.5 * density * (velocity_x * velocity_x + velocity_y * velocity_y + velocity_z * velocity_z)
    return jnp.stack([density, density * velocity_x, density * velocity_y, density * velocity_z, energy]).astype(jnp.float32)


def draw_coarse(key, part):
    return conserved(jax.random.fold_in(key, 11), (NXC, NZC, NYC))


def draw_fine(key, part):
    return conserved(jax.random.fold_in(key, 23), (PATCHES, P_SIZE, P_SIZE * P_SIZE))


def draw_columns(key, part):
    chosen = jax.random.permutation(jax.random.fold_in(key, 37), GY * GZ)[:PYZ]
    return jnp.stack([chosen % GY, chosen // GY], axis=1).astype(jnp.int32)


def setup_inputs(seed: int = 0) -> dict:
    seeds = jax.random.split(jax.random.key(seed), 5)
    return {
        "coarse": draw_coarse(jax.random.fold_in(seeds[4], 71), 0),
        "fine": draw_fine(jax.random.fold_in(seeds[4], 71), 0),
        "columns": draw_columns(jax.random.fold_in(seeds[4], 71), 0),
        "patch_ids": jax.vmap(lambda own: jax.random.permutation(own, SLOTS))(jax.random.split(seeds[3], N_SLAB)).reshape((N_SLAB, SLOTS)).astype(jnp.int32),
    }


heat_ratio = 1.4
fine_rate = 0.1
coarse_rate = 0.05

def euler_flux(fields, normal_axis):
    density = fields[0]
    momentum = fields[1:4]
    energy = fields[4]
    velocity = momentum / density
    pressure = (heat_ratio - 1.0) * (energy - 0.5 * lax.optimization_barrier(jnp.sum(momentum * velocity, axis=0)))
    normal_speed = velocity[normal_axis]
    components = [momentum[normal_axis], momentum[0] * normal_speed, momentum[1] * normal_speed, momentum[2] * normal_speed, (energy + pressure) * normal_speed]
    components[1 + normal_axis] = components[1 + normal_axis] + pressure
    signal = jnp.abs(normal_speed) + jnp.sqrt(heat_ratio * pressure / density)
    return (jnp.stack(components), signal)

def rusanov(left_side, right_side, normal_axis):
    left_flux, left_signal = euler_flux(left_side, normal_axis)
    right_flux, right_signal = euler_flux(right_side, normal_axis)
    return 0.5 * (left_flux + right_flux) - 0.5 * jnp.maximum(left_signal, right_signal) * (right_side - left_side)

def advance(fields, ghosts):
    x_low, x_high, z_low, z_high, y_low, y_high = ghosts
    along_x = jnp.concatenate([x_low[:, :, None], fields, x_high[:, :, None]], axis=2)
    flux_x = rusanov(along_x[:, :, :-1], along_x[:, :, 1:], 0)
    along_z = jnp.concatenate([z_low[:, :, :, None], fields, z_high[:, :, :, None]], axis=3)
    flux_z = rusanov(along_z[:, :, :, :-1], along_z[:, :, :, 1:], 2)
    along_y = jnp.concatenate([y_low[..., None], fields, y_high[..., None]], axis=4)
    flux_y = rusanov(along_y[..., :-1], along_y[..., 1:], 1)
    change = flux_x[:, :, 1:] - flux_x[:, :, :-1] + (flux_z[:, :, :, 1:] - flux_z[:, :, :, :-1]) + (flux_y[..., 1:] - flux_y[..., :-1])
    updated = fields - fine_rate * change
    return (updated, (flux_y[..., 0], flux_y[..., -1], flux_z[:, :, :, 0], flux_z[:, :, :, -1]))

def pair_mean(face_cells):
    extents = face_cells.shape
    return face_cells.reshape(extents[0], extents[1], extents[2] // 2, 2, extents[3] // 2, 2).mean(axis=(3, 5))

def cell_mean(fields):
    extents = fields.shape
    return fields.reshape(extents[0], extents[1], extents[2] // 2, 2, extents[3] // 2, 2, extents[4] // 2, 2).mean(axis=(3, 5, 7))

def upsample(face_cells):
    return jnp.repeat(jnp.repeat(face_cells, 2, axis=-2), 2, axis=-1)

def onehot(indices, extent):
    return (indices[:, None] == jnp.arange(extent, dtype=jnp.int32)[None, :]).astype(jnp.float32)

def neighbours(columns, step_y, step_z):
    matches = (columns[None, :, 0] == columns[:, None, 0] + step_y) & (columns[None, :, 1] == columns[:, None, 1] + step_z)
    present = jnp.any(matches, axis=1)
    partner = lax.optimization_barrier(jnp.sum(jnp.where(matches, jnp.arange(columns.shape[0], dtype=jnp.int32)[None, :], 0), axis=1)).astype(jnp.int32)
    return (present, partner)

def block_targets(column_y, column_z):
    grid_width = GY + 2
    return ((column_z + 1) * grid_width + column_y + 1, (column_z + 1) * grid_width + column_y, (column_z + 1) * grid_width + column_y + 2, column_z * grid_width + column_y + 1, (column_z + 2) * grid_width + column_y + 1)

def cover_mask(columns):
    centre = block_targets(columns[:, 0], columns[:, 1])[0]
    occupied = lax.optimization_barrier(jnp.sum(onehot(centre, (GZ + 2) * (GY + 2)), axis=0))
    return jnp.repeat(jnp.repeat(occupied.reshape(GZ + 2, GY + 2), H, axis=0), H, axis=1)

def block_form(slab):
    layer_depth = slab.shape[1] // H
    shaped = slab.reshape(5, layer_depth, H, GZ + 2, H, GY + 2, H).transpose(0, 1, 2, 4, 6, 3, 5)
    return shaped.reshape(5, layer_depth, H, H, H, (GZ + 2) * (GY + 2))

def slab_form(blocks):
    layer_depth = blocks.shape[1]
    shaped = blocks.reshape(5, layer_depth, H, H, H, GZ + 2, GY + 2).transpose(0, 1, 2, 5, 3, 6, 4)
    return shaped.reshape(5, layer_depth * H, (GZ + 2) * H, (GY + 2) * H)

def reorder(slab_fields, order_index):
    return jnp.take(slab_fields, order_index, axis=1)

def arrange(values):
    return jnp.moveaxis(jnp.moveaxis(values, 0, 1), 2, -1)

def reference(coarse, fine, columns, patch_ids):
    layers = N_SLAB * LX
    slot_count = LX * PYZ
    slot_range = jnp.arange(slot_count, dtype=jnp.int32)
    inverse = lax.optimization_barrier(jnp.sum(jnp.where(patch_ids[:, :, None] == slot_range[None, None, :], slot_range[None, :, None], 0), axis=1)).astype(jnp.int32)
    grouped = fine.reshape(5, N_SLAB, slot_count, P_SIZE, P_SIZE, P_SIZE)
    ordered = jax.vmap(reorder, in_axes=(1, 0), out_axes=1)(grouped, inverse)
    fields_all = ordered.reshape(5, layers, PYZ, P_SIZE, P_SIZE, P_SIZE)
    x_lower = jnp.concatenate([fields_all[:, :1, :, 0], fields_all[:, :-1, :, P_SIZE - 1]], axis=1)
    x_upper = jnp.concatenate([fields_all[:, 1:, :, 0], fields_all[:, -1:, :, P_SIZE - 1]], axis=1)
    column_y = columns[:, 0]
    column_z = columns[:, 1]
    centre, below_y, above_y, below_z, above_z = block_targets(column_y, column_z)
    blocks = block_form(coarse)

    def inject(portion, target):
        return upsample(jnp.moveaxis(jnp.take(portion, target, axis=4), 4, 2))

    def blend_faces(step_y, step_z, neighbour_face, coarse_face):
        present, partner = neighbours(columns, step_y, step_z)
        return jnp.where(present[None, None, :, None, None], jnp.take(neighbour_face, partner, axis=2), coarse_face)
    y_lower_ghost = blend_faces(-1, 0, fields_all[..., P_SIZE - 1], inject(blocks[:, :, :, :, H - 1], below_y))
    y_upper_ghost = blend_faces(1, 0, fields_all[..., 0], inject(blocks[:, :, :, :, 0], above_y))
    z_lower_ghost = blend_faces(0, -1, fields_all[:, :, :, :, P_SIZE - 1], inject(blocks[:, :, :, H - 1], below_z))
    z_upper_ghost = blend_faces(0, 1, fields_all[:, :, :, :, 0], inject(blocks[:, :, :, 0], above_z))

    def layer_step(member):
        updated, boundary = advance(member[0], member[1:])
        return (updated, cell_mean(updated), tuple((pair_mean(face_cells) for face_cells in boundary)))
    members = tuple((jnp.moveaxis(source, 1, 0) for source in (fields_all, x_lower, x_upper, z_lower_ghost, z_upper_ghost, y_lower_ghost, y_upper_ghost)))
    updated, averaged, boundary = lax.map(layer_step, members)
    by_number = jnp.moveaxis(updated, 0, 1).reshape(5, N_SLAB, slot_count, P_SIZE, P_SIZE, P_SIZE)
    fine_out = jax.vmap(reorder, in_axes=(1, 0), out_axes=1)(by_number, patch_ids).reshape(5, N_SLAB * slot_count, P_SIZE, P_SIZE * P_SIZE)

    def absent_mask(step_y, step_z):
        return 1.0 - neighbours(columns, step_y, step_z)[0].astype(jnp.float32)
    y_lower = -coarse_rate * arrange(boundary[0]) * absent_mask(-1, 0)
    y_upper = coarse_rate * arrange(boundary[1]) * absent_mask(1, 0)
    z_lower = -coarse_rate * arrange(boundary[2]) * absent_mask(0, -1)
    z_upper = coarse_rate * arrange(boundary[3]) * absent_mask(0, 1)
    first_row = (jnp.arange(H) == 0).astype(jnp.float32)
    last_row = (jnp.arange(H) == H - 1).astype(jnp.float32)
    nblocks = (GZ + 2) * (GY + 2)
    totals = jnp.zeros((5, layers, H, H, H, nblocks), jnp.float32)
    totals = totals.at[..., centre].add(arrange(averaged))
    totals = totals.at[..., below_y].add(y_lower[:, :, :, :, None, :] * last_row[:, None])
    totals = totals.at[..., above_y].add(y_upper[:, :, :, :, None, :] * first_row[:, None])
    totals = totals.at[..., below_z].add(z_lower[:, :, :, None, :, :] * last_row[:, None, None])
    totals = totals.at[..., above_z].add(z_upper[:, :, :, None, :, :] * first_row[:, None, None])
    contrib = slab_form(totals)
    covered = cover_mask(columns)
    along_x = jnp.concatenate([coarse[:, :1], coarse, coarse[:, -1:]], axis=1)
    along_z = jnp.concatenate([coarse[:, :, :1], coarse, coarse[:, :, -1:]], axis=2)
    along_y = jnp.concatenate([coarse[..., :1], coarse, coarse[..., -1:]], axis=3)
    cover_z = jnp.pad(covered, ((1, 1), (0, 0)))
    cover_y = jnp.pad(covered, ((0, 0), (1, 1)))
    flux_x = rusanov(along_x[:, :-1], along_x[:, 1:], 0) * (1.0 - covered)
    flux_z = rusanov(along_z[:, :, :-1], along_z[:, :, 1:], 2) * ((1.0 - cover_z[:-1]) * (1.0 - cover_z[1:]))
    flux_y = rusanov(along_y[..., :-1], along_y[..., 1:], 1) * ((1.0 - cover_y[:, :-1]) * (1.0 - cover_y[:, 1:]))
    change = flux_x[:, 1:] - flux_x[:, :-1] + (flux_z[:, :, 1:] - flux_z[:, :, :-1]) + (flux_y[..., 1:] - flux_y[..., :-1])
    provisional = coarse - coarse_rate * change
    coarse_out = jnp.where(covered > 0, contrib, provisional + contrib)
    return (coarse_out, fine_out)
```

```python
import functools

import jax
import jax.numpy as jnp
from jax import lax
from jax.experimental import pallas as pl
from jax.experimental.pallas import tpu as pltpu
from jax.sharding import PartitionSpec as P

LANES = 128
heat_ratio = 1.4
fine_rate = 0.1
coarse_rate = 0.05
VMEM = pl.BlockSpec(memory_space=pltpu.VMEM)
SMEM = pl.BlockSpec(memory_space=pltpu.SMEM)


def up8(count):
    return -(-count // 8) * 8


class Sizes:
    def __init__(self, n, slabs, fine_shape, coarse_shape, slots):
        self.n, self.slabs, self.S = n, slabs, slots
        self.own = fine_shape[1]
        self.P = fine_shape[2]
        self.cells = fine_shape[3]
        self.H = self.P // 2
        self.G = self.cells // LANES
        self.zg = LANES // self.P
        self.xa = self.P // n
        self.xc = self.H // n
        self.PL = self.cells // n
        self.zcl = self.P // n // 2
        self.NX, self.R, self.NY = coarse_shape[1:]
        self.m = self.H // self.R
        self.NZ = self.R * n
        self.lines = 2 * (self.NY // self.H)
        assert self.NX == self.H and self.NY == LANES and self.H % self.R == 0
        assert self.P % (2 * n) == 0 and 4 * self.P == LANES and slots == self.own * n
        self.lat = 5 * self.xa * self.own
        self.ny = -(-(5 * self.xc * self.R) // LANES)
        self.OY = up8(self.lat)
        self.OZ = self.OY + self.lines * self.ny
        self.RC = up8(self.OZ + 10 * self.xc)
        self.RX = up8(10 * self.own)
        self.RA = 5 * self.H
        self.OFX = self.lat
        self.RF = up8(self.lat + 10 * self.own)
        self.OXQ = 5 * self.xc * self.R
        self.RK = up8(self.OXQ + 10 * self.zcl)
        self.RM = 5 * self.R + 8


def parts(x, count):
    out = []
    for _ in range(count):
        piece = x.astype(jnp.bfloat16)
        out.append(piece)
        x = x - piece.astype(jnp.float32)
    return out


def select_dot(pick, x, count=3, dims=(((1,), (0,)), ((), ()))):
    total = None
    for piece in parts(x, count):
        term = lax.dot_general(pick, piece, dims, preferred_element_type=jnp.float32)
        total = term if total is None else total + term
    return total


def lanes_at(x, index):
    return jnp.take_along_axis(x, index, axis=1, mode="promise_in_bounds")


def derived(U):
    inverse = 1.0 / U[0]
    velocity = [U[1] * inverse, U[2] * inverse, U[3] * inverse]
    kinetic = U[1] * velocity[0] + U[2] * velocity[1] + U[3] * velocity[2]
    pressure = (heat_ratio - 1.0) * (U[4] - 0.5 * kinetic)
    sound = jnp.sqrt(heat_ratio * pressure * inverse)
    return velocity, pressure, sound


def directed(U, speed, pressure, d):
    out = [U[0] * speed if d is None else U[1 + d]]
    out += [U[1 + e] * speed + (pressure if e == d else 0.0) if e == d else U[1 + e] * speed for e in range(3)]
    out.append((U[4] + pressure) * speed)
    return out


def twice_flux(L, dl, R, dr, d):
    fl = directed(L, dl[0], dl[1], d)
    fr = directed(R, dr[0], dr[1], d)
    signal = jnp.maximum(jnp.abs(dl[0]) + dl[2], jnp.abs(dr[0]) + dr[2])
    return [fl[v] + fr[v] - signal * (R[v] - L[v]) for v in range(5)]


def state_flux(L, R, d):
    vl, pl_, cl = derived(L)
    vr, pr, cr = derived(R)
    return twice_flux(L, (vl[d], pl_, cl), R, (vr[d], pr, cr), d)


def extract_kernel(z, fine, coarse, number_row, com, xf, up, dn, pu, pd, scr):
    lane = lax.broadcasted_iota(jnp.int32, (z.P, LANES), 1)
    pick = z.P * ((lane % z.P) % z.zg) + jnp.where(lane >= 3 * z.P, z.P - 1, 0)
    group = jnp.where(lane >= 2 * z.P, (lane % z.P) // z.zg, -1)
    for q in range(z.own):
        for v in range(5):
            first = fine[v, q, :, :LANES]
            last = fine[v, q, :, (z.G - 1) * LANES :]
            face = jnp.where(lane < z.P, first, pltpu.roll(last, 2 * z.P, 1))
            for g in range(z.G):
                chunk = fine[v, q, :, g * LANES : (g + 1) * LANES]
                face = jnp.where(group == g, lanes_at(chunk, pick), face)
            scr[v % 2] = face
            for a in range(z.xa):
                com[pl.ds((v * z.xa + a) * z.own + q, z.n, stride=z.RC), :] = scr[v % 2, pl.ds(a, z.n, stride=z.xa), :]
            for side in range(2):
                row = fine[v, q, side * (z.P - 1) : side * (z.P - 1) + 1, :]
                place = (side * 5 + v) * z.own + q
                for j in range(z.n):
                    xf[j * z.RX + place : j * z.RX + place + 1, : z.PL] = row[:, j * z.PL : (j + 1) * z.PL]
    line = lax.broadcasted_iota(jnp.int32, (z.lines, LANES), 0)
    at = lax.broadcasted_iota(jnp.int32, (z.lines, LANES), 1)
    chosen = (at == z.H * (line // 2) + (z.H - 1) * (line % 2)).astype(jnp.bfloat16)
    width = 5 * z.xc * z.R
    for j in range(z.n):
        block = coarse[:, j * z.xc : (j + 1) * z.xc].reshape(width, LANES)
        lines = select_dot(chosen, block, 3, (((1,), (1,)), ((), ())))
        for t in range(z.ny):
            extent = min(LANES, width - t * LANES)
            com[j * z.RC + z.OY + t * z.lines : j * z.RC + z.OY + (t + 1) * z.lines, :extent] = lines[
                :, t * LANES : t * LANES + extent
            ]
        for v in range(5):
            for x in range(z.xc):
                row = j * z.RC + z.OZ + (v * z.xc + x) * 2
                com[row : row + 1, :] = coarse[v, j * z.xc + x, 0:1, :]
                com[row + 1 : row + 2, :] = coarse[v, j * z.xc + x, z.R - 1 : z.R, :]
    for v in range(5):
        up[v * z.R : (v + 1) * z.R, :] = coarse[v, z.NX - 1]
        dn[v * z.R : (v + 1) * z.R, :] = coarse[v, 0]
        for x in range(z.NX):
            row = v * z.NX + x
            pu[row : row + 1, :] = coarse[v, x, z.R - 1 : z.R, :]
            pd[row : row + 1, :] = coarse[v, x, 0:1, :]
    numbers = jnp.broadcast_to(number_row[...], (8, LANES))
    up[5 * z.R : 5 * z.R + 8, :] = numbers
    dn[5 * z.R : 5 * z.R + 8, :] = numbers


def advance_kernel(z, fine, updated, avg, der, zflux, sums):
    lane = lax.broadcasted_iota(jnp.int32, (z.P, LANES), 1)
    row = lax.broadcasted_iota(jnp.int32, (z.P, LANES), 0)
    inner_x = row < z.P - 1
    inner_y = lane % z.P < z.P - 1
    high = lane >= LANES - z.P

    def first_pass(step, carry):
        q = step // z.G
        g = step % z.G
        at = pl.ds(pl.multiple_of(g * LANES, LANES), LANES)
        U = [fine[v, q, :, at] for v in range(5)]
        velocity, pressure, sound = derived(U)
        for k, value in enumerate(velocity + [pressure, sound]):
            der[k, q, :, at] = value
        return carry

    lax.fori_loop(0, z.own * z.G, first_pass, 0)

    def second_pass(step, carry):
        q = step // z.G
        g = step % z.G
        at = pl.ds(pl.multiple_of(g * LANES, LANES), LANES)
        nxt = pl.ds(pl.multiple_of(jnp.minimum(g + 1, z.G - 1) * LANES, LANES), LANES)
        U = [fine[v, q, :, at] for v in range(5)]
        D = [der[k, q, :, at] for k in range(5)]
        change = None
        for d in (0, 1):
            if d == 0:
                move = lambda a: pltpu.roll(a, z.P - 1, 0)
                back = lambda a: pltpu.roll(a, 1, 0)
                inner = inner_x
            else:
                move = lambda a: pltpu.roll(a, LANES - 1, 1)
                back = lambda a: pltpu.roll(a, 1, 1)
                inner = inner_y
            f = directed(U, D[d], D[3], d)
            s = jnp.abs(D[d]) + D[4]
            signal = jnp.maximum(s, move(s))
            up = []
            for v in range(5):
                face = f[v] + move(f[v]) - signal * (move(U[v]) - U[v])
                face = jnp.where(inner, face, 0.0)
                up.append(face - back(face))
            change = up if change is None else [change[v] + up[v] for v in range(5)]
        f = directed(U, D[2], D[3], 2)
        s = jnp.abs(D[2]) + D[4]
        UN = [fine[v, q, :, nxt] for v in range(5)]
        DN = [der[k, q, :, nxt] for k in (2, 3, 4)]
        fn = directed(UN, DN[0], DN[1], 2)
        sn = jnp.abs(DN[0]) + DN[2]
        beyond = lambda a, b: jnp.where(high, pltpu.roll(b, LANES - z.P, 1), pltpu.roll(a, LANES - z.P, 1))
        signal = jnp.maximum(s, beyond(s, sn))
        inner_z = jnp.logical_or(lane < LANES - z.P, g < z.G - 1)
        for v in range(5):
            face = f[v] + beyond(f[v], fn[v]) - signal * (beyond(U[v], UN[v]) - U[v])
            face = jnp.where(inner_z, face, 0.0)
            rolled = pltpu.roll(face, z.P, 1)
            before = jnp.where(g == 0, 0.0, zflux[v])
            zflux[v] = rolled
            total = change[v] + (face - jnp.where(lane < z.P, before, rolled))
            new = U[v] - (0.5 * fine_rate) * total
            updated[v, q, :, at] = new
            sums[pl.ds(pl.multiple_of(((v * z.own + q) * z.G + g) * z.P, z.P), z.P), :] = new
        return carry

    lax.fori_loop(0, z.own * z.G, second_pass, 0)
    spot = lax.broadcasted_iota(jnp.int32, (z.n, LANES), 1)
    half = z.zg // 2

    def average(step, carry):
        v = step // z.G
        g = step % z.G
        out = [jnp.zeros((z.n, LANES), jnp.float32) for _ in range(half)]
        for q in range(z.own):
            base = pl.multiple_of(((v * z.own + q) * z.G + g) * z.P, z.P)
            for x in range(z.xc):
                pair = sums[pl.ds(base + 2 * x, z.n, stride=z.xa), :] + sums[pl.ds(base + 2 * x + 1, z.n, stride=z.xa), :]
                pair = pair + pltpu.roll(pair, LANES - 1, 1)
                pair = pair + pltpu.roll(pair, LANES - z.P, 1)
                for h in range(half):
                    out[h] = jnp.where(
                        spot // z.H == x * z.own + q, lanes_at(pair, 2 * z.P * h + 2 * (spot % z.H)), out[h]
                    )
        for h in range(half):
            avg[pl.ds(v * z.H + half * g + h, z.n, stride=z.RA), :] = 0.125 * out[h]
        return carry

    lax.fori_loop(0, 5 * z.G, average, 0)


def coverage(columns, block_z, block_y, count):
    def step(k, found):
        return jnp.logical_or(found, (block_y == columns[k, 0] + 1) & (block_z == columns[k, 1] + 1)).astype(jnp.int32)

    return lax.fori_loop(0, count, step, jnp.zeros(block_z.shape, jnp.int32))


def provisional_kernel(z, info, columns, coarse, below, above, lower, upper, out, pad):
    slab, rank = info[0], info[1]
    row = lax.broadcasted_iota(jnp.int32, (z.R, LANES), 0)
    lane = lax.broadcasted_iota(jnp.int32, (z.R, LANES), 1)
    place = row + rank * z.R
    block = lambda a: (a + z.H) // z.H - 1
    count = columns.shape[0]
    cover = lambda dz, dy: coverage(columns, block(place + dz), block(lane + dy), count)
    own, zu, zd, yu, yd = [1.0 - cover(*s).astype(jnp.float32) for s in ((0, 0), (1, 0), (-1, 0), (0, 1), (0, -1))]
    for v in range(5):
        pad[v, 1 : z.NX + 1] = coarse[v]
        pad[v, 0] = jnp.where(slab == 0, coarse[v, 0], below[v * z.R : (v + 1) * z.R, :])
        pad[v, z.NX + 1] = jnp.where(slab == z.slabs - 1, coarse[v, z.NX - 1], above[v * z.R : (v + 1) * z.R, :])

    def layer(x, carry):
        U = [pad[v, x + 1] for v in range(5)]
        XL = [pad[v, x] for v in range(5)]
        XU = [pad[v, x + 2] for v in range(5)]
        ZL, ZU, YL, YU = [], [], [], []
        for v in range(5):
            low = jnp.where(rank == 0, U[v][0:1], lower[pl.ds(v * z.NX + x, 1), :])
            top = jnp.where(rank == z.n - 1, U[v][z.R - 1 :], upper[pl.ds(v * z.NX + x, 1), :])
            ZL.append(jnp.where(row == 0, low, pltpu.roll(U[v], 1, 0)))
            ZU.append(jnp.where(row == z.R - 1, top, pltpu.roll(U[v], z.R - 1, 0)))
            YL.append(jnp.where(lane == 0, U[v], pltpu.roll(U[v], 1, 1)))
            YU.append(jnp.where(lane == LANES - 1, U[v], pltpu.roll(U[v], LANES - 1, 1)))
        fx = [a - b for a, b in zip(state_flux(U, XU, 0), state_flux(XL, U, 0))]
        fz = [a * zu - b * zd for a, b in zip(state_flux(U, ZU, 2), state_flux(ZL, U, 2))]
        fy = [a * yu - b * yd for a, b in zip(state_flux(U, YU, 1), state_flux(YL, U, 1))]
        for v in range(5):
            value = U[v] - (0.5 * coarse_rate) * (fx[v] + fz[v] + fy[v])
            out[v, x] = jnp.where(own > 0.0, value, 0.0)
        return carry

    lax.fori_loop(0, z.NX, layer, 0)


def middle_kernel(z, info, spots, ctab, rtab, com, xo, xb, xu, below, above, avg, outf, outc, lat, ghost, xs, canvas):
    slab = info[0]
    S, f_of = z.S, z.P
    gy, gz, number = ctab[:, 0:1], ctab[:, 1:2], ctab[:, 2:3]
    gyr, gzr = rtab[0:1, :], rtab[1:2, :]
    lane = lax.broadcasted_iota(jnp.int32, (S, LANES), 1)
    kind = lane // f_of
    even = kind % 2 == 0
    steps = ((0, -1), (0, 1), (-1, 0), (1, 0))
    flags = [((gyr == gy + dy) & (gzr == gz + dz)).astype(jnp.float32) for dy, dz in steps]
    turned = [((gy == gyr + dy) & (gz == gzr + dz)).astype(jnp.float32) for dy, dz in steps]
    absent_row = [1.0 - jnp.sum(t, axis=0, keepdims=True) for t in turned]
    here = jnp.zeros((S, LANES), jnp.float32)
    for k in range(4):
        here = jnp.where(kind == k, jnp.sum(flags[k], axis=1, keepdims=True), here)
    picks = jnp.concatenate(flags, axis=1).astype(jnp.bfloat16)

    for i in range(z.n):
        for k in range(5 * z.xa):
            lat[k * S + i * z.own : k * S + (i + 1) * z.own, :] = com[i * z.RC + k * z.own : i * z.RC + (k + 1) * z.own, :]

    def onehot(index, extent):
        return (lax.broadcasted_iota(jnp.int32, (S, extent), 1) == index).astype(jnp.bfloat16)

    vx = 5 * z.xc
    low_lines = jnp.concatenate([com[pl.ds(z.OZ + 2 * k + 1, z.n, stride=z.RC), :] for k in range(vx)], axis=1)
    top_lines = jnp.concatenate([com[pl.ds(z.OZ + 2 * k, z.n, stride=z.RC), :] for k in range(vx)], axis=1)
    low_rows = select_dot(onehot(gz * z.m + z.m - 1, z.n), low_lines)
    top_rows = select_dot(onehot((gz + 2) * z.m, z.n), top_lines)
    y_index = z.H * (gy + 1) + (lane % f_of) // 2
    half = (lane % f_of) // 2
    y_rows = {}
    for t in range(z.ny):
        table = jnp.concatenate(
            [com[i * z.RC + z.OY + t * z.lines : i * z.RC + z.OY + (t + 1) * z.lines, :] for i in range(z.n)], axis=0
        )
        for h in range(z.m):
            for f, line in ((2, 2 * gy + 1), (3, 2 * (gy + 2))):
                y_rows[t, h, f] = select_dot(onehot(((gz + 1) * z.m + h) * z.lines + line, z.n * z.lines), table)
    for v in range(5):
        swapped = []
        for a in range(z.xa):
            T = lat[(v * z.xa + a) * S : (v * z.xa + a + 1) * S, :]
            T = jnp.where(even, pltpu.roll(T, LANES - f_of, 1), pltpu.roll(T, f_of, 1))
            swapped.append(jnp.concatenate([jnp.where(kind == k, T, 0.0) for k in range(4)], axis=0))
        near = select_dot(picks, jnp.concatenate(swapped, axis=1))
        for x in range(z.xc):
            k = v * z.xc + x
            at = slice(k * LANES, (k + 1) * LANES)
            c = jnp.where(kind == 0, lanes_at(low_rows[:, at], y_index), lanes_at(top_rows[:, at], y_index))
            start = k * z.R
            for f in (2, 3):
                for h in range(z.m):
                    got = lanes_at(y_rows[start // LANES, h, f], start % LANES + half % z.R)
                    c = jnp.where((kind == f) & (half // z.R == h), got, c)
            for a in (2 * x, 2 * x + 1):
                ghost[(v * z.xa + a) * S : (v * z.xa + a + 1) * S, :] = jnp.where(
                    here > 0.0, near[:, a * LANES : (a + 1) * LANES], c
                )

    is_z = kind < 2
    sign = jnp.where(even, 0.5 * fine_rate, -0.5 * fine_rate)
    for a in range(z.xa):
        at = [slice((v * z.xa + a) * S, (v * z.xa + a + 1) * S) for v in range(5)]
        own = [lat[s, :] for s in at]
        far = [ghost[s, :] for s in at]
        L = [jnp.where(even, far[v], own[v]) for v in range(5)]
        R = [jnp.where(even, own[v], far[v]) for v in range(5)]
        vl, pl_, cl = derived(L)
        vr, pr, cr = derived(R)
        sl = jnp.where(is_z, vl[2], vl[1])
        sr = jnp.where(is_z, vr[2], vr[1])
        F = twice_flux(L, (sl, pl_, cl), R, (sr, pr, cr), None)
        both = pl_ + pr
        F[2] = F[2] + jnp.where(is_z, 0.0, both)
        F[3] = F[3] + jnp.where(is_z, both, 0.0)
        for v in range(5):
            C = sign * F[v]
            ghost[at[v], :] = C
            for d in range(z.n):
                k = d * z.RF + (v * z.xa + a) * z.own
                outf[k : k + z.own, :] = C[d * z.own : (d + 1) * z.own]

    zrow = lax.broadcasted_iota(jnp.int32, (z.NZ, S), 0)
    base = z.H * (gzr + 1)
    zmat = jnp.concatenate(
        [
            (zrow == base).astype(jnp.float32) - absent_row[0] * (zrow == base - 1).astype(jnp.float32),
            (zrow == base + z.H - 1).astype(jnp.float32) - absent_row[1] * (zrow == base + z.H).astype(jnp.float32),
        ],
        axis=1,
    ).astype(jnp.bfloat16)
    ybase = z.H * (gy + 1)
    absent = [1.0 - jnp.sum(flags[k], axis=1, keepdims=True) for k in (2, 3)]
    ymat = jnp.concatenate(
        [
            (lane == ybase).astype(jnp.float32) - absent[0] * (lane == ybase - 1).astype(jnp.float32),
            (lane == ybase + z.H - 1).astype(jnp.float32) - absent[1] * (lane == ybase + z.H).astype(jnp.float32),
        ],
        axis=0,
    ).astype(jnp.bfloat16)
    in_y = lane // z.H == gy + 1
    in_z = lane // z.H == gz + 1
    for v in range(5):
        for x in range(z.xc):
            k = v * z.xc + x
            r = (v * z.xa + 2 * x) * S
            Q = ghost[r : r + S, :] + ghost[r + S : r + 2 * S, :]
            Q = 0.125 * (Q + pltpu.roll(Q, LANES - 1, 1))
            got = [lanes_at(Q, f_of * f + 2 * (lane % z.H)) for f in range(4)]
            zq = jnp.concatenate([jnp.where(in_y, got[f], 0.0) for f in (0, 1)], axis=0)
            yq = jnp.concatenate([jnp.where(in_z, got[f], 0.0) for f in (2, 3)], axis=0)
            total = select_dot(zmat, zq, 2)
            for piece in parts(yq.T, 2):
                total = total + jnp.dot(piece, ymat, preferred_element_type=jnp.float32)
            canvas[k * z.NZ : (k + 1) * z.NZ, :] = total

    spot = lax.broadcasted_iota(jnp.int32, (z.H, LANES), 1) // z.H

    def place(k, carry):
        i = k // z.own
        q = k % z.own
        sy = spots[0, k] + 1
        sz = spots[1, k] + 1
        inside = spot == sy
        for v in range(5):
            block = avg[pl.ds(pl.multiple_of(i * z.RA + v * z.H, 8), z.H), :]
            for x in range(z.xc):
                shift = lax.rem(z.H * (sy - (x * z.own + q)) + 2 * LANES, LANES)
                rows = pl.ds(pl.multiple_of((v * z.xc + x) * z.NZ + z.H * sz, z.H), z.H)
                canvas[rows, :] = canvas[rows, :] + jnp.where(inside, pltpu.roll(block, shift, 1), 0.0)
        return carry

    lax.fori_loop(0, S, place, 0)
    for d in range(z.n):
        for k in range(vx):
            outc[d * z.RK + k * z.R : d * z.RK + (k + 1) * z.R, :] = canvas[k * z.NZ + d * z.R : k * z.NZ + (d + 1) * z.R, :]

    tables = ((xo, 0), (xo, 5), (xb, 5), (xu, 0))
    for w, (source, offset) in enumerate(tables):
        for i in range(z.n):
            for v in range(5):
                k = (w * 5 + v) * S + i * z.own
                r = i * z.RX + (offset + v) * z.own
                xs[k : k + z.own, :] = source[r : r + z.own, :]
    value = number.astype(jnp.float32)
    zb = (
        lax.broadcasted_iota(jnp.int32, (z.n, S), 0) // z.m == gzr + 1
    ).astype(jnp.bfloat16)
    for side, (margin, edge) in enumerate(((below, slab == 0), (above, slab == z.slabs - 1))):
        match = (value == margin[5 * z.R : 5 * z.R + 1, :S]).astype(jnp.bfloat16)
        own = [xs[(side * 5 + v) * S : (side * 5 + v + 1) * S, :] for v in range(5)]
        far = select_dot(
            match, jnp.concatenate([xs[((2 + side) * 5 + v) * S : ((2 + side) * 5 + v + 1) * S, :] for v in range(5)], axis=1)
        )
        far = [jnp.where(edge, own[v], far[:, v * LANES : (v + 1) * LANES]) for v in range(5)]
        F = state_flux(far, own, 0) if side == 0 else state_flux(own, far, 0)
        for v in range(5):
            C = (0.5 * fine_rate if side == 0 else -0.5 * fine_rate) * F[v]
            for d in range(z.n):
                k = d * z.RF + z.OFX + (side * 5 + v) * z.own
                outf[k : k + z.own, :] = C[d * z.own : (d + 1) * z.own]
            Q = C + pltpu.roll(C, LANES - 1, 1)
            Q = 0.125 * (Q + pltpu.roll(Q, LANES - z.P, 1))
            for h in range(z.zcl):
                got = jnp.where(in_y, lanes_at(Q, 2 * z.P * h + 2 * (lane % z.H)), 0.0)
                outc[pl.ds(z.OXQ + (v * 2 + side) * z.zcl + h, z.n, stride=z.RK), :] = select_dot(zb, got, 2)


def fine_kernel(z, updated, recv, out, scr):
    lane = lax.broadcasted_iota(jnp.int32, (z.P, LANES), 1)
    y = lane % z.P
    edge = (y == 0) | (y == z.P - 1)
    pick = jnp.where(y == 0, 2 * z.P, 3 * z.P) + lane // z.P
    for v in range(5):
        for q in range(z.own):
            for a in range(z.xa):
                scr[q % 2, pl.ds(a, z.n, stride=z.xa), :] = recv[pl.ds((v * z.xa + a) * z.own + q, z.n, stride=z.RF), :]
            face = scr[q % 2]
            for g in range(z.G):
                at = slice(g * LANES, (g + 1) * LANES)
                add = jnp.where(edge, lanes_at(face, jnp.where(edge, pick + z.zg * g, 0)), 0.0)
                if g == 0:
                    add = add + jnp.where(lane < z.P, face, 0.0)
                if g == z.G - 1:
                    add = add + jnp.where(lane >= LANES - z.P, pltpu.roll(face, 2 * z.P, 1), 0.0)
                out[v, q, :, at] = updated[v, q, :, at] + add
            for side in range(2):
                x = side * (z.P - 1)
                for j in range(z.n):
                    r = j * z.RF + z.OFX + (side * 5 + v) * z.own + q
                    at = slice(j * z.PL, (j + 1) * z.PL)
                    out[v, q, x : x + 1, at] = out[v, q, x : x + 1, at] + recv[r : r + 1, : z.PL]


def coarse_kernel(z, info, prov, recv, out):
    for j in range(z.n):
        for v in range(5):
            for x in range(z.xc):
                r = j * z.RK + (v * z.xc + x) * z.R
                out[v, j * z.xc + x] = prov[v, j * z.xc + x] + recv[r : r + z.R, :]
    offset = 0 if z.m == 1 else lax.rem(info[1], z.m) * z.R
    for v in range(5):
        for side in range(2):
            x = side * (z.NX - 1)
            for zl in range(z.R):
                zc = zl + offset
                r = (zc // z.zcl) * z.RK + z.OXQ + (v * 2 + side) * z.zcl + zc % z.zcl
                out[v, x, zl : zl + 1, :] = out[v, x, zl : zl + 1, :] + recv[pl.ds(r, 1), :]


def call(kernel, z, outs, ins, scratch=(), aliases=None, name=None):
    return pl.pallas_call(
        functools.partial(kernel, z),
        out_shape=[jax.ShapeDtypeStruct(s, jnp.float32) for s in outs],
        in_specs=[SMEM if space == "s" else VMEM for space, _ in ins],
        out_specs=[VMEM] * len(outs),
        scratch_shapes=[pltpu.VMEM(s, jnp.float32) for s in scratch],
        input_output_aliases=aliases or {},
        compiler_params=pltpu.CompilerParams(vmem_limit_bytes=56 * 1024 * 1024),
        name=name,
    )(*[a for _, a in ins])


def local(n, slabs, coarse, fine, columns, patch_ids):
    numbers = patch_ids[0]
    slots = numbers.shape[0]
    assert columns.shape[0] == slots
    z = Sizes(n, slabs, fine.shape, coarse.shape, slots)
    info = jnp.stack([lax.axis_index("slab"), lax.axis_index("patch")]).astype(jnp.int32)
    held = numbers[:, None] == jnp.arange(slots, dtype=jnp.int32)[None, :]
    spots = jnp.sum(jnp.where(held[None], columns.T[:, None, :], 0), axis=2).astype(jnp.int32)
    rtab = jnp.concatenate([spots, numbers[None]], axis=0)
    ctab = rtab.T
    number_row = jnp.pad(numbers.astype(jnp.float32), (0, LANES - slots))[None]

    exchange = lambda a: lax.all_to_all(a, "patch", 0, 0, tiled=True)
    ahead = lambda count: [(i, i + 1) for i in range(count - 1)]
    back = lambda count: [(i + 1, i) for i in range(count - 1)]

    com, xf, up, dn, pu, pd = call(
        extract_kernel,
        z,
        [(n * z.RC, LANES), (n * z.RX, LANES), (z.RM, LANES), (z.RM, LANES), (5 * z.NX, LANES), (5 * z.NX, LANES)],
        [("v", fine), ("v", coarse), ("v", number_row)],
        [(2, z.P, LANES)],
        name="extract",
    )
    xo = exchange(xf)
    below = lax.ppermute(up, "slab", ahead(slabs))
    above = lax.ppermute(dn, "slab", back(slabs))
    lower = lax.ppermute(pu, "patch", ahead(n))
    upper = lax.ppermute(pd, "patch", back(n))
    xb = lax.ppermute(xo, "slab", ahead(slabs))
    xu = lax.ppermute(xo, "slab", back(slabs))
    com = exchange(com)
    updated, avg = call(
        advance_kernel,
        z,
        [fine.shape, (n * z.RA, LANES)],
        [("v", fine)],
        [fine.shape, (5, z.P, LANES), (5 * z.own * z.G * z.P, LANES)],
        name="advance",
    )
    avg = exchange(avg)
    (prov,) = call(
        provisional_kernel,
        z,
        [coarse.shape],
        [("s", info), ("s", columns), ("v", coarse), ("v", below), ("v", above), ("v", lower), ("v", upper)],
        [(5, z.NX + 2, z.R, LANES)],
        name="provisional",
    )
    outf, outc = call(
        middle_kernel,
        z,
        [(n * z.RF, LANES), (n * z.RK, LANES)],
        [("s", info), ("s", spots), ("v", ctab), ("v", rtab)]
        + [("v", a) for a in (com, xo, xb, xu, below, above, avg)],
        [(5 * z.xa * slots, LANES), (5 * z.xa * slots, LANES), (20 * slots, LANES), (5 * z.xc * z.NZ, LANES)],
        name="middle",
    )
    outf = exchange(outf)
    outc = exchange(outc)
    (fine_out,) = call(
        fine_kernel, z, [fine.shape], [("v", updated), ("v", outf)], [(2, z.P, LANES)], {0: 0}, name="fine_edges"
    )
    (coarse_out,) = call(
        coarse_kernel, z, [coarse.shape], [("s", info), ("v", prov), ("v", outc)], name="coarse_sum"
    )
    return coarse_out, fine_out


def solution(mesh):
    n, slabs = mesh.shape["patch"], mesh.shape["slab"]
    return jax.shard_map(
        functools.partial(local, n, slabs),
        mesh=mesh,
        in_specs=(
            P(None, "slab", "patch", None),
            P(None, ("slab", "patch"), None, None),
            P(),
            P("slab", None),
        ),
        out_specs=(P(None, "slab", "patch", None), P(None, ("slab", "patch"), None, None)),
        check_vma=False,
    )
```

```python
import functools

import jax
import jax.numpy as jnp
from jax import lax
from jax.experimental import pallas as pl
from jax.experimental.pallas import tpu as pltpu
from jax.sharding import PartitionSpec as P


LANES = 128
XROWS = 16
heat_ratio = 1.4
fine_rate = 0.1
coarse_rate = 0.05
VMEM = pl.BlockSpec(memory_space=pltpu.VMEM)
SMEM = pl.BlockSpec(memory_space=pltpu.SMEM)


def up8(count):
    return -(-count // 8) * 8


class Sizes:
    def __init__(self, n, slabs, fine_shape, coarse_shape, slots):
        self.n, self.slabs, self.S = n, slabs, slots
        self.own = fine_shape[1]
        self.P = fine_shape[2]
        self.cells = fine_shape[3]
        self.H = self.P // 2
        self.G = self.cells // LANES
        self.zg = LANES // self.P
        self.xa = self.P // n
        self.xc = self.H // n
        self.PL = self.cells // n
        self.zcl = self.P // n // 2
        self.NX, self.R, self.NY = coarse_shape[1:]
        self.m = self.H // self.R
        self.NZ = self.R * n
        self.lines = 2 * (self.NY // self.H)
        assert self.NX == self.H and self.NY == LANES and self.H % self.R == 0
        assert self.P % (2 * n) == 0 and 4 * self.P == LANES and slots == self.own * n
        self.lat = 5 * self.xa * self.own
        self.ny = -(-(5 * self.xc * self.R) // LANES)
        self.OY = up8(self.lat)
        self.OZ = self.OY + self.lines * self.ny
        self.OX = self.OZ + 10 * self.xc
        self.RC = up8(self.OX + 10 * self.own)
        self.OM = up8(n * 5 * self.own)
        self.RA = 5 * self.H
        self.OFX = self.lat
        self.RF = up8(self.lat + 10 * self.own)
        self.OXQ = 5 * self.xc * self.R
        self.RK = up8(self.OXQ + 10 * self.zcl)
        self.RM = 5 * self.R + 8
        self.RP = self.OM + self.RM


def parts(x, count):
    out = []
    for _ in range(count):
        piece = x.astype(jnp.bfloat16)
        out.append(piece)
        x = x - piece.astype(jnp.float32)
    return out


def select_dot(pick, x, count=3, dims=(((1,), (0,)), ((), ()))):
    total = None
    for piece in parts(x, count):
        term = lax.dot_general(pick, piece, dims, preferred_element_type=jnp.float32)
        total = term if total is None else total + term
    return total


def lanes_at(x, index):
    return jnp.take_along_axis(x, index, axis=1, mode="promise_in_bounds")


def derived(U):
    inverse = 1.0 / U[0]
    velocity = [U[1] * inverse, U[2] * inverse, U[3] * inverse]
    kinetic = U[1] * velocity[0] + U[2] * velocity[1] + U[3] * velocity[2]
    pressure = (heat_ratio - 1.0) * (U[4] - 0.5 * kinetic)
    sound = jnp.sqrt(heat_ratio * pressure * inverse)
    return velocity, pressure, sound


def directed(U, speed, pressure, d):
    out = [U[0] * speed if d is None else U[1 + d]]
    out += [U[1 + e] * speed + (pressure if e == d else 0.0) if e == d else U[1 + e] * speed for e in range(3)]
    out.append((U[4] + pressure) * speed)
    return out


def twice_flux(L, dl, R, dr, d):
    fl = directed(L, dl[0], dl[1], d)
    fr = directed(R, dr[0], dr[1], d)
    signal = jnp.maximum(jnp.abs(dl[0]) + dl[2], jnp.abs(dr[0]) + dr[2])
    return [fl[v] + fr[v] - signal * (R[v] - L[v]) for v in range(5)]


def state_flux(L, R, d):
    vl, pl_, cl = derived(L)
    vr, pr, cr = derived(R)
    return twice_flux(L, (vl[d], pl_, cl), R, (vr[d], pr, cr), d)


def positions(z, ids, columns):
    down = lax.broadcasted_iota(jnp.int32, (z.S, z.S), 0)
    across = lax.broadcasted_iota(jnp.int32, (z.S, z.S), 1)
    number_row = ids[...].astype(jnp.float32)
    held = down.astype(jnp.float32) == number_row
    place = columns[...].astype(jnp.float32)
    rows = [jnp.sum(jnp.where(held, place[:, k : k + 1], 0.0), axis=0, keepdims=True) for k in range(2)]
    turn = lambda r: jnp.sum(jnp.where(down == across, r, 0.0), axis=1, keepdims=True)
    whole = lambda a: a.astype(jnp.int32)
    return turn(number_row), whole(turn(rows[0])), whole(turn(rows[1])), whole(rows[0]), whole(rows[1])


def extract_kernel(z, fine, coarse, com, scr):
    lane = lax.broadcasted_iota(jnp.int32, (z.P, LANES), 1)
    pick = z.P * ((lane % z.P) % z.zg) + jnp.where(lane >= 3 * z.P, z.P - 1, 0)
    group = jnp.where(lane >= 2 * z.P, (lane % z.P) // z.zg, -1)
    for q in range(z.own):
        for v in range(5):
            first = fine[v, q, :, :LANES]
            last = fine[v, q, :, (z.G - 1) * LANES :]
            face = jnp.where(lane < z.P, first, pltpu.roll(last, 2 * z.P, 1))
            for g in range(z.G):
                chunk = fine[v, q, :, g * LANES : (g + 1) * LANES]
                face = jnp.where(group == g, lanes_at(chunk, pick), face)
            scr[v % 2] = face
            for a in range(z.xa):
                com[pl.ds((v * z.xa + a) * z.own + q, z.n, stride=z.RC), :] = scr[v % 2, pl.ds(a, z.n, stride=z.xa), :]
            for side in range(2):
                row = fine[v, q, side * (z.P - 1) : side * (z.P - 1) + 1, :]
                place = z.OX + (side * 5 + v) * z.own + q
                for j in range(z.n):
                    com[j * z.RC + place : j * z.RC + place + 1, : z.PL] = row[:, j * z.PL : (j + 1) * z.PL]
    line = lax.broadcasted_iota(jnp.int32, (z.lines, LANES), 0)
    at = lax.broadcasted_iota(jnp.int32, (z.lines, LANES), 1)
    chosen = (at == z.H * (line // 2) + (z.H - 1) * (line % 2)).astype(jnp.bfloat16)
    width = 5 * z.xc * z.R
    for j in range(z.n):
        block = coarse[:, j * z.xc : (j + 1) * z.xc].reshape(width, LANES)
        lines = select_dot(chosen, block, 3, (((1,), (1,)), ((), ())))
        for t in range(z.ny):
            extent = min(LANES, width - t * LANES)
            com[j * z.RC + z.OY + t * z.lines : j * z.RC + z.OY + (t + 1) * z.lines, :extent] = lines[
                :, t * LANES : t * LANES + extent
            ]
        for v in range(5):
            for x in range(z.xc):
                row = j * z.RC + z.OZ + (v * z.xc + x) * 2
                com[row : row + 1, :] = coarse[v, j * z.xc + x, 0:1, :]
                com[row + 1 : row + 2, :] = coarse[v, j * z.xc + x, z.R - 1 : z.R, :]


def pack_kernel(z, com, coarse, ids, up, dn):
    for side, margin, layer in ((1, up, z.NX - 1), (0, dn, 0)):
        for i in range(z.n):
            k = i * z.RC + z.OX + side * 5 * z.own
            margin[i * 5 * z.own : (i + 1) * 5 * z.own, :] = com[k : k + 5 * z.own, :]
        for v in range(5):
            margin[z.OM + v * z.R : z.OM + (v + 1) * z.R, :] = coarse[v, layer]
        margin[z.OM + 5 * z.R : z.OM + 5 * z.R + 8, :] = jnp.zeros((8, LANES), jnp.float32)
        margin[z.OM + 5 * z.R : z.OM + 5 * z.R + 1, : z.S] = ids[...].astype(jnp.float32)


def advance_kernel(z, fine, updated, avg, work, xflux, zflux, sums):
    count = z.own
    patch = pl.program_id(0)
    X = min(XROWS, z.P)
    lane = lax.broadcasted_iota(jnp.int32, (X, LANES), 1)
    row = lax.broadcasted_iota(jnp.int32, (X, LANES), 0)
    inner_y = lane % z.P < z.P - 1
    first_z = lane < z.P

    def first_pass(i, carry):
        at = pl.ds(pl.multiple_of(i * LANES, LANES), LANES)
        U = [fine[v, 0, :, at] for v in range(5)]
        velocity, pressure, sound = derived(U)
        for k, value in enumerate(U + velocity + [pressure, sound]):
            work[k, i, : z.P, :] = value
        return carry

    lax.fori_loop(0, z.G, first_pass, 0)
    xflux[:, :8, :] = jnp.zeros((5, 8, LANES), jnp.float32)

    def second_pass(i, carry):
        at = pl.ds(pl.multiple_of(i * LANES, LANES), LANES)
        nxt = jnp.minimum(i + 1, z.G - 1)
        inner_z = jnp.logical_or(lane < LANES - z.P, i < z.G - 1)
        for r in range(0, z.P, X):
            rows = slice(r, r + X)
            U = [work[k, i, rows, :] for k in range(5)]
            D = [work[k, i, rows, :] for k in range(5, 10)]
            XU = [work[k, i, r + 1 : r + 1 + X, :] for k in range(5)]
            XD = [work[k, i, r + 1 : r + 1 + X, :] for k in (5, 8, 9)]
            F = twice_flux(U, (D[0], D[3], D[4]), XU, XD, 0)
            change = []
            for v in range(5):
                face = jnp.where(row < z.P - 1 - r, F[v], 0.0) if r + X == z.P else F[v]
                xflux[v, 8 + r : 8 + r + X, :] = face
                change.append(face - xflux[v, 7 + r : 7 + r + X, :])
            ahead = lambda a: pltpu.roll(a, LANES - 1, 1)
            F = twice_flux(U, (D[1], D[3], D[4]), [ahead(a) for a in U], [ahead(D[k]) for k in (1, 3, 4)], 1)
            for v in range(5):
                face = jnp.where(inner_y, F[v], 0.0)
                change[v] = change[v] + (face - pltpu.roll(face, 1, 1))
            beyond = lambda k, a: pltpu.roll(jnp.where(first_z, work[k, nxt, rows, :], a), LANES - z.P, 1)
            F = twice_flux(
                U,
                (D[2], D[3], D[4]),
                [beyond(k, U[k]) for k in range(5)],
                [beyond(5 + k, D[k]) for k in (2, 3, 4)],
                2,
            )
            for v in range(5):
                face = jnp.where(inner_z, F[v], 0.0)
                rolled = pltpu.roll(face, z.P, 1)
                before = jnp.where(i == 0, 0.0, zflux[v, rows, :])
                zflux[v, rows, :] = rolled
                new = U[v] - (0.5 * fine_rate) * (change[v] + (face - jnp.where(first_z, before, rolled)))
                updated[v, 0, rows, at] = new
                sums[v, patch * z.G + i, rows, :] = new
        return carry

    lax.fori_loop(0, z.G, second_pass, 0)

    @pl.when(patch == count - 1)
    def _():
        half = z.zg // 2
        depth = z.xc * count * LANES
        source = lax.broadcasted_iota(jnp.int32, (depth, half * LANES), 0)
        target = lax.broadcasted_iota(jnp.int32, (depth, half * LANES), 1)
        place = source % LANES
        piece = source // LANES
        mean = (
            (piece == (target % LANES) // z.H)
            & (place // (2 * z.P) == target // LANES)
            & ((place % z.P) // 2 == target % z.H)
        )
        mean = jnp.where(mean, 0.125, 0.0).astype(jnp.bfloat16)

        def average(v, carry):
            columns = []
            for x in range(z.xc):
                for q in range(count):
                    blocks = []
                    for g in range(z.G):
                        i = q * z.G + g
                        blocks.append(
                            sums[v, i, pl.ds(2 * x, z.n, stride=z.xa), :] + sums[v, i, pl.ds(2 * x + 1, z.n, stride=z.xa), :]
                        )
                    columns.append(jnp.concatenate(blocks, axis=0))
            lhs = jnp.concatenate(parts(jnp.concatenate(columns, axis=1), 3), axis=0)
            got = jnp.dot(lhs, mean, preferred_element_type=jnp.float32)
            lines = z.G * z.n
            got = got[:lines] + got[lines : 2 * lines] + got[2 * lines :]
            for g in range(z.G):
                for h in range(half):
                    rows = pl.ds(v * z.H + half * g + h, z.n, stride=z.RA)
                    value = got[g * z.n : (g + 1) * z.n, h * LANES : (h + 1) * LANES]
                    avg[rows, :] = value
            return carry

        lax.fori_loop(0, 5, average, 0)


def coverage(columns, block_z, block_y, count):
    def step(k, found):
        return jnp.logical_or(found, (block_y == columns[k, 0] + 1) & (block_z == columns[k, 1] + 1)).astype(jnp.int32)

    return lax.fori_loop(0, count, step, jnp.zeros(block_z.shape, jnp.int32))


def provisional_kernel(z, columns, coarse, below, above, out, pad):
    slab, rank = lax.axis_index("slab"), lax.axis_index("patch")
    row = lax.broadcasted_iota(jnp.int32, (z.R, LANES), 0)
    lane = lax.broadcasted_iota(jnp.int32, (z.R, LANES), 1)
    place = row + rank * z.R
    block = lambda a: (a + z.H) // z.H - 1
    count = columns.shape[0]
    cover = lambda dz, dy: coverage(columns, block(place + dz), block(lane + dy), count)
    own, zu, zd, yu, yd = [1.0 - cover(*s).astype(jnp.float32) for s in ((0, 0), (1, 0), (-1, 0), (0, 1), (0, -1))]
    zu = jnp.where(row < z.R - 1, zu, 0.0)
    zd = jnp.where(row > 0, zd, 0.0)
    for v in range(5):
        pad[v, 1 : z.NX + 1] = coarse[v]
        pad[v, 0] = jnp.where(slab == 0, coarse[v, 0], below[z.OM + v * z.R : z.OM + (v + 1) * z.R, :])
        pad[v, z.NX + 1] = jnp.where(slab == z.slabs - 1, coarse[v, z.NX - 1], above[z.OM + v * z.R : z.OM + (v + 1) * z.R, :])

    def layer(x, carry):
        U = [pad[v, x + 1] for v in range(5)]
        XL = [pad[v, x] for v in range(5)]
        XU = [pad[v, x + 2] for v in range(5)]
        ZL = [pltpu.roll(U[v], 1, 0) for v in range(5)]
        ZU = [pltpu.roll(U[v], z.R - 1, 0) for v in range(5)]
        YL = [jnp.where(lane == 0, U[v], pltpu.roll(U[v], 1, 1)) for v in range(5)]
        YU = [jnp.where(lane == LANES - 1, U[v], pltpu.roll(U[v], LANES - 1, 1)) for v in range(5)]
        fx = [a - b for a, b in zip(state_flux(U, XU, 0), state_flux(XL, U, 0))]
        fz = [a * zu - b * zd for a, b in zip(state_flux(U, ZU, 2), state_flux(ZL, U, 2))]
        fy = [a * yu - b * yd for a, b in zip(state_flux(U, YU, 1), state_flux(YL, U, 1))]
        for v in range(5):
            value = U[v] - (0.5 * coarse_rate) * (fx[v] + fz[v] + fy[v])
            out[v, x] = jnp.where(own > 0.0, value, 0.0)
        return carry

    lax.fori_loop(0, z.NX, layer, 0)


def side_kernel(z, ids, columns, com, ghost, lat):
    S, f_of = z.S, z.P
    _, gy, gz, gyr, gzr = positions(z, ids, columns)
    lane = lax.broadcasted_iota(jnp.int32, (S, LANES), 1)
    kind = lane // f_of
    even = kind % 2 == 0
    steps = ((0, -1), (0, 1), (-1, 0), (1, 0))
    flags = [((gyr == gy + dy) & (gzr == gz + dz)).astype(jnp.float32) for dy, dz in steps]
    here = jnp.zeros((S, LANES), jnp.float32)
    for k in range(4):
        here = jnp.where(kind == k, jnp.sum(flags[k], axis=1, keepdims=True), here)
    picks = jnp.concatenate(flags, axis=1).astype(jnp.bfloat16)

    for i in range(z.n):
        for k in range(5 * z.xa):
            lat[k * S + i * z.own : k * S + (i + 1) * z.own, :] = com[i * z.RC + k * z.own : i * z.RC + (k + 1) * z.own, :]

    def onehot(index, extent):
        return (lax.broadcasted_iota(jnp.int32, (S, extent), 1) == index).astype(jnp.bfloat16)

    vx = 5 * z.xc
    low_lines = jnp.concatenate([com[pl.ds(z.OZ + 2 * k + 1, z.n, stride=z.RC), :] for k in range(vx)], axis=1)
    top_lines = jnp.concatenate([com[pl.ds(z.OZ + 2 * k, z.n, stride=z.RC), :] for k in range(vx)], axis=1)
    low_rows = select_dot(onehot(gz * z.m + z.m - 1, z.n), low_lines)
    top_rows = select_dot(onehot((gz + 2) * z.m, z.n), top_lines)
    y_index = z.H * (gy + 1) + (lane % f_of) // 2
    half = (lane % f_of) // 2
    y_rows = {}
    for t in range(z.ny):
        table = jnp.concatenate(
            [com[i * z.RC + z.OY + t * z.lines : i * z.RC + z.OY + (t + 1) * z.lines, :] for i in range(z.n)], axis=0
        )
        for h in range(z.m):
            for f, line in ((2, 2 * gy + 1), (3, 2 * (gy + 2))):
                y_rows[t, h, f] = select_dot(onehot(((gz + 1) * z.m + h) * z.lines + line, z.n * z.lines), table)
    for v in range(5):
        swapped = []
        for a in range(z.xa):
            T = lat[(v * z.xa + a) * S : (v * z.xa + a + 1) * S, :]
            T = jnp.where(even, pltpu.roll(T, LANES - f_of, 1), pltpu.roll(T, f_of, 1))
            swapped.append(jnp.concatenate([jnp.where(kind == k, T, 0.0) for k in range(4)], axis=0))
        near = select_dot(picks, jnp.concatenate(swapped, axis=1))
        for x in range(z.xc):
            k = v * z.xc + x
            at = slice(k * LANES, (k + 1) * LANES)
            c = jnp.where(kind == 0, lanes_at(low_rows[:, at], y_index), lanes_at(top_rows[:, at], y_index))
            start = k * z.R
            for f in (2, 3):
                for h in range(z.m):
                    got = lanes_at(y_rows[start // LANES, h, f], start % LANES + half % z.R)
                    c = jnp.where((kind == f) & (half // z.R == h), got, c)
            for a in (2 * x, 2 * x + 1):
                ghost[(v * z.xa + a) * S : (v * z.xa + a + 1) * S, :] = jnp.where(
                    here > 0.0, near[:, a * LANES : (a + 1) * LANES], c
                )

    is_z = kind < 2
    sign = jnp.where(even, 0.5 * fine_rate, -0.5 * fine_rate)
    for a in range(z.xa):
        at = [slice((v * z.xa + a) * S, (v * z.xa + a + 1) * S) for v in range(5)]
        own = [lat[s, :] for s in at]
        far = [ghost[s, :] for s in at]
        L = [jnp.where(even, far[v], own[v]) for v in range(5)]
        R = [jnp.where(even, own[v], far[v]) for v in range(5)]
        vl, pl_, cl = derived(L)
        vr, pr, cr = derived(R)
        sl = jnp.where(is_z, vl[2], vl[1])
        sr = jnp.where(is_z, vr[2], vr[1])
        F = twice_flux(L, (sl, pl_, cl), R, (sr, pr, cr), None)
        both = pl_ + pr
        F[2] = F[2] + jnp.where(is_z, 0.0, both)
        F[3] = F[3] + jnp.where(is_z, both, 0.0)
        for v in range(5):
            C = sign * F[v]
            ghost[at[v], :] = C


def end_kernel(z, ids, columns, com, ghost, below, above, outf, xc, xs):
    S = z.S
    slab = lax.axis_index("slab")
    number = positions(z, ids, columns)[0]
    for d in range(z.n):
        for k in range(5 * z.xa):
            outf[d * z.RF + k * z.own : d * z.RF + (k + 1) * z.own, :] = ghost[k * S + d * z.own : k * S + (d + 1) * z.own, :]
    for w, (source, pitch, offset) in enumerate(
        ((com, z.RC, z.OX), (com, z.RC, z.OX + 5 * z.own), (below, 5 * z.own, 0), (above, 5 * z.own, 0))
    ):
        for i in range(z.n):
            for v in range(5):
                k = (w * 5 + v) * S + i * z.own
                r = i * pitch + offset + v * z.own
                xs[k : k + z.own, :] = source[r : r + z.own, :]
    for side, (margin, edge) in enumerate(((below, slab == 0), (above, slab == z.slabs - 1))):
        match = (number == margin[z.OM + 5 * z.R : z.OM + 5 * z.R + 1, :S]).astype(jnp.bfloat16)
        own = [xs[(side * 5 + v) * S : (side * 5 + v + 1) * S, :] for v in range(5)]
        far = select_dot(
            match, jnp.concatenate([xs[((2 + side) * 5 + v) * S : ((2 + side) * 5 + v + 1) * S, :] for v in range(5)], axis=1)
        )
        far = [jnp.where(edge, own[v], far[:, v * LANES : (v + 1) * LANES]) for v in range(5)]
        F = state_flux(far, own, 0) if side == 0 else state_flux(own, far, 0)
        for v in range(5):
            C = (0.5 * fine_rate if side == 0 else -0.5 * fine_rate) * F[v]
            xc[(side * 5 + v) * S : (side * 5 + v + 1) * S, :] = C
            for d in range(z.n):
                k = d * z.RF + z.OFX + (side * 5 + v) * z.own
                outf[k : k + z.own, :] = C[d * z.own : (d + 1) * z.own]


def canvas_kernel(z, ids_s, columns_s, ids, columns, com, ghost, xc, avg, outc, canvas):
    S, f_of = z.S, z.P
    vx = 5 * z.xc
    _, gy, gz, gyr, gzr = positions(z, ids, columns)
    lane = lax.broadcasted_iota(jnp.int32, (S, LANES), 1)
    steps = ((0, -1), (0, 1), (-1, 0), (1, 0))
    flags = [((gyr == gy + dy) & (gzr == gz + dz)).astype(jnp.float32) for dy, dz in steps]
    turned = [((gy == gyr + dy) & (gz == gzr + dz)).astype(jnp.float32) for dy, dz in steps]
    absent_row = [1.0 - jnp.sum(t, axis=0, keepdims=True) for t in turned]
    zrow = lax.broadcasted_iota(jnp.int32, (z.NZ, S), 0)
    base = z.H * (gzr + 1)
    zmat = jnp.concatenate(
        [
            (zrow == base).astype(jnp.float32) - absent_row[0] * (zrow == base - 1).astype(jnp.float32),
            (zrow == base + z.H - 1).astype(jnp.float32) - absent_row[1] * (zrow == base + z.H).astype(jnp.float32),
        ],
        axis=1,
    ).astype(jnp.bfloat16)
    ybase = z.H * (gy + 1)
    absent = [1.0 - jnp.sum(flags[k], axis=1, keepdims=True) for k in (2, 3)]
    ymat = jnp.concatenate(
        [
            (lane == ybase).astype(jnp.float32) - absent[0] * (lane == ybase - 1).astype(jnp.float32),
            (lane == ybase + z.H - 1).astype(jnp.float32) - absent[1] * (lane == ybase + z.H).astype(jnp.float32),
        ],
        axis=0,
    ).astype(jnp.bfloat16)
    in_y = lane // z.H == gy + 1
    in_z = lane // z.H == gz + 1
    for v in range(5):
        for x in range(z.xc):
            k = v * z.xc + x
            r = (v * z.xa + 2 * x) * S
            Q = ghost[r : r + S, :] + ghost[r + S : r + 2 * S, :]
            Q = 0.125 * (Q + pltpu.roll(Q, LANES - 1, 1))
            got = [lanes_at(Q, f_of * f + 2 * (lane % z.H)) for f in range(4)]
            zq = jnp.concatenate([jnp.where(in_y, got[f], 0.0) for f in (0, 1)], axis=0)
            yq = jnp.concatenate([jnp.where(in_z, got[f], 0.0) for f in (2, 3)], axis=0)
            total = select_dot(zmat, zq, 2)
            for piece in parts(yq.T, 2):
                total = total + jnp.dot(piece, ymat, preferred_element_type=jnp.float32)
            canvas[k * z.NZ : (k + 1) * z.NZ, :] = total

    rank = lax.broadcasted_iota(jnp.int32, (z.n, LANES), 0)
    rank_slot = lax.broadcasted_iota(jnp.int32, (z.n, S), 0)
    inside_y = in_y.astype(jnp.bfloat16)
    cover = lambda block: jnp.dot((block == gzr + 1).astype(jnp.bfloat16), inside_y, preferred_element_type=jnp.float32)
    bare_first = 1.0 - cover((rank_slot * z.R) // z.H)
    bare_last = 1.0 - cover((rank_slot * z.R + z.R - 1) // z.H)
    low_mask = bare_first * jnp.where(rank == 0, 1.0, pltpu.roll(bare_last, 1, 0))
    top_mask = bare_last * jnp.where(rank == z.n - 1, 1.0, pltpu.roll(bare_first, z.n - 1, 0))
    for x in range(z.xc):
        lines = [[com[pl.ds(z.OZ + 2 * (v * z.xc + x) + s, z.n, stride=z.RC), :] for v in range(5)] for s in (0, 1)]
        under = [jnp.where(rank == 0, lines[0][v], pltpu.roll(lines[1][v], 1, 0)) for v in range(5)]
        over = [jnp.where(rank == z.n - 1, lines[1][v], pltpu.roll(lines[0][v], z.n - 1, 0)) for v in range(5)]
        low = state_flux(under, lines[0], 2)
        top = state_flux(lines[1], over, 2)
        for v in range(5):
            first = pl.ds((v * z.xc + x) * z.NZ, z.n, stride=z.R)
            last = pl.ds((v * z.xc + x) * z.NZ + z.R - 1, z.n, stride=z.R)
            canvas[first, :] = canvas[first, :] + (0.5 * coarse_rate) * low_mask * low[v]
            canvas[last, :] = canvas[last, :] - (0.5 * coarse_rate) * top_mask * top[v]

    spot = lax.broadcasted_iota(jnp.int32, (z.H, LANES), 1) // z.H

    def place(k, carry):
        i = k // z.own
        q = k % z.own
        sy = columns_s[ids_s[0, k], 0] + 1
        sz = columns_s[ids_s[0, k], 1] + 1
        inside = spot == sy
        for v in range(5):
            block = avg[pl.ds(pl.multiple_of(i * z.RA + v * z.H, 8), z.H), :]
            for x in range(z.xc):
                shift = lax.rem(z.H * (sy - (x * z.own + q)) + 2 * LANES, LANES)
                rows = pl.ds(pl.multiple_of((v * z.xc + x) * z.NZ + z.H * sz, z.H), z.H)
                canvas[rows, :] = canvas[rows, :] + jnp.where(inside, pltpu.roll(block, shift, 1), 0.0)
        return carry

    lax.fori_loop(0, S, place, 0)
    for d in range(z.n):
        for k in range(vx):
            outc[d * z.RK + k * z.R : d * z.RK + (k + 1) * z.R, :] = canvas[k * z.NZ + d * z.R : k * z.NZ + (d + 1) * z.R, :]


    zb = (rank_slot // z.m == gzr + 1).astype(jnp.bfloat16)
    for side in range(2):
        for v in range(5):
            C = xc[(side * 5 + v) * S : (side * 5 + v + 1) * S, :]
            Q = C + pltpu.roll(C, LANES - 1, 1)
            Q = 0.125 * (Q + pltpu.roll(Q, LANES - z.P, 1))
            for h in range(z.zcl):
                got = jnp.where(in_y, lanes_at(Q, 2 * z.P * h + 2 * (lane % z.H)), 0.0)
                outc[pl.ds(z.OXQ + (v * 2 + side) * z.zcl + h, z.n, stride=z.RK), :] = select_dot(zb, got, 2)


def fine_kernel(z, updated, recv, out, scr):
    lane = lax.broadcasted_iota(jnp.int32, (z.P, LANES), 1)
    y = lane % z.P
    edge = (y == 0) | (y == z.P - 1)
    pick = jnp.where(y == 0, 2 * z.P, 3 * z.P) + lane // z.P
    for v in range(5):
        for q in range(z.own):
            for a in range(z.xa):
                scr[q % 2, pl.ds(a, z.n, stride=z.xa), :] = recv[pl.ds((v * z.xa + a) * z.own + q, z.n, stride=z.RF), :]
            face = scr[q % 2]
            for g in range(z.G):
                at = slice(g * LANES, (g + 1) * LANES)
                add = jnp.where(edge, lanes_at(face, jnp.where(edge, pick + z.zg * g, 0)), 0.0)
                if g == 0:
                    add = add + jnp.where(lane < z.P, face, 0.0)
                if g == z.G - 1:
                    add = add + jnp.where(lane >= LANES - z.P, pltpu.roll(face, 2 * z.P, 1), 0.0)
                out[v, q, :, at] = updated[v, q, :, at] + add
            for side in range(2):
                x = side * (z.P - 1)
                for j in range(z.n):
                    r = j * z.RF + z.OFX + (side * 5 + v) * z.own + q
                    at = slice(j * z.PL, (j + 1) * z.PL)
                    out[v, q, x : x + 1, at] = out[v, q, x : x + 1, at] + recv[r : r + 1, : z.PL]


def coarse_kernel(z, prov, recv, out):
    for j in range(z.n):
        for v in range(5):
            for x in range(z.xc):
                r = j * z.RK + (v * z.xc + x) * z.R
                out[v, j * z.xc + x] = prov[v, j * z.xc + x] + recv[r : r + z.R, :]
    offset = 0 if z.m == 1 else lax.rem(lax.axis_index("patch"), z.m) * z.R
    for v in range(5):
        for side in range(2):
            x = side * (z.NX - 1)
            for zl in range(z.R):
                zc = zl + offset
                r = (zc // z.zcl) * z.RK + z.OXQ + (v * 2 + side) * z.zcl + zc % z.zcl
                out[v, x, zl : zl + 1, :] = out[v, x, zl : zl + 1, :] + recv[pl.ds(r, 1), :]


def call(kernel, z, outs, ins, scratch=(), aliases=None):
    return pl.pallas_call(
        functools.partial(kernel, z),
        out_shape=[jax.ShapeDtypeStruct(s, jnp.float32) for s in outs],
        in_specs=[SMEM if space == "s" else VMEM for space, _ in ins],
        out_specs=[VMEM] * len(outs),
        scratch_shapes=[pltpu.VMEM(s, jnp.float32) for s in scratch],
        input_output_aliases=aliases or {},
        compiler_params=pltpu.CompilerParams(vmem_limit_bytes=56 * 1024 * 1024),
    )(*[a for _, a in ins])


def run_advance(z, fine):
    block = pl.BlockSpec((5, 1) + fine.shape[2:], lambda i: (0, i, 0, 0))
    average = (z.n * z.RA, LANES)
    return pl.pallas_call(
        functools.partial(advance_kernel, z),
        grid=(z.own,),
        out_shape=[jax.ShapeDtypeStruct(fine.shape, jnp.float32), jax.ShapeDtypeStruct(average, jnp.float32)],
        in_specs=[block],
        out_specs=[block, pl.BlockSpec(average, lambda i: (0, 0))],
        scratch_shapes=[
            pltpu.VMEM(s, jnp.float32)
            for s in ((10, z.G, z.P + 8, LANES), (5, z.P + 8, LANES), (5, z.P, LANES), (5, z.own * z.G, z.P, LANES))
        ],
        compiler_params=pltpu.CompilerParams(vmem_limit_bytes=56 * 1024 * 1024),
        name="advance",
    )(fine)


def local(n, slabs, coarse, fine, columns, patch_ids):
    return level_step(n, slabs, coarse, fine, columns, patch_ids)


def level_step(n, slabs, coarse, fine, columns, patch_ids):
    slots = patch_ids.shape[1]
    assert columns.shape[0] == slots
    z = Sizes(n, slabs, fine.shape, coarse.shape, slots)

    def exchange(a):
        return lax.all_to_all(a, "patch", 0, 0, tiled=True)

    def shifted(a, step):
        pairs = [(i, i + step) for i in range(slabs) if 0 <= i + step < slabs]
        return lax.ppermute(a, "slab", pairs)

    faces = (5 * z.xa * slots, LANES)
    (com,) = call(extract_kernel, z, [(n * z.RC, LANES)], [("v", fine), ("v", coarse)], [(2, z.P, LANES)])
    com = exchange(com)
    updated, avg = run_advance(z, fine)
    avg = exchange(avg)
    up, dn = call(pack_kernel, z, [(z.RP, LANES)] * 2, [("v", com), ("v", coarse), ("v", patch_ids)])
    below = shifted(up, 1)
    above = shifted(dn, -1)
    (ghost,) = call(side_kernel, z, [faces], [("v", a) for a in (patch_ids, columns, com)], [faces])
    outf, xc = call(
        end_kernel,
        z,
        [(n * z.RF, LANES), (10 * slots, LANES)],
        [("v", a) for a in (patch_ids, columns, com, ghost, below, above)],
        [(20 * slots, LANES)],
    )
    outf = exchange(outf)
    (prov,) = call(
        provisional_kernel,
        z,
        [coarse.shape],
        [("s", columns), ("v", coarse), ("v", below), ("v", above)],
        [(5, z.NX + 2, z.R, LANES)],
    )
    (outc,) = call(
        canvas_kernel,
        z,
        [(n * z.RK, LANES)],
        [("s", patch_ids), ("s", columns)] + [("v", a) for a in (patch_ids, columns, com, ghost, xc, avg)],
        [(5 * z.xc * z.NZ, LANES)],
    )
    outc = exchange(outc)
    (fine_out,) = call(fine_kernel, z, [fine.shape], [("v", updated), ("v", outf)], [(2, z.P, LANES)])
    (coarse_out,) = call(coarse_kernel, z, [coarse.shape], [("v", prov), ("v", outc)])
    return coarse_out, fine_out


def solution(mesh):
    n, slabs = mesh.shape["patch"], mesh.shape["slab"]
    return jax.shard_map(
        functools.partial(local, n, slabs),
        mesh=mesh,
        in_specs=(
            P(None, "slab", "patch", None),
            P(None, ("slab", "patch"), None, None),
            P(),
            P("slab", None),
        ),
        out_specs=(P(None, "slab", "patch", None), P(None, ("slab", "patch"), None, None)),
        check_vma=False,
    )
```

```python
import functools

import jax
import jax.numpy as jnp
from jax import lax
from jax.experimental import pallas as pl
from jax.experimental.pallas import tpu as pltpu
from jax.sharding import PartitionSpec as P


LANES = 128
XROWS = 16
VMEM_LIMIT = 24 * 1024 * 1024
heat_ratio = 1.4
fine_rate = 0.1
coarse_rate = 0.05
VMEM = pl.BlockSpec(memory_space=pltpu.VMEM)
SMEM = pl.BlockSpec(memory_space=pltpu.SMEM)


def up8(count):
    return -(-count // 8) * 8


class Sizes:
    def __init__(self, n, slabs, fine_shape, coarse_shape, slots):
        self.n, self.slabs, self.S = n, slabs, slots
        self.own = fine_shape[1]
        self.P = fine_shape[2]
        self.cells = fine_shape[3]
        self.H = self.P // 2
        self.G = self.cells // LANES
        self.zg = LANES // self.P
        self.xa = self.P // n
        self.xc = self.H // n
        self.PL = self.cells // n
        self.zcl = self.P // n // 2
        self.NX, self.R, self.NY = coarse_shape[1:]
        self.m = self.H // self.R
        self.NZ = self.R * n
        self.lines = 2 * (self.NY // self.H)
        assert self.NX == self.H and self.NY == LANES and self.H % self.R == 0
        assert self.P % (2 * n) == 0 and 4 * self.P == LANES and slots == self.own * n
        self.lat = 5 * self.xa * self.own
        self.ny = -(-(5 * self.xc * self.R) // LANES)
        self.OY = up8(self.lat)
        self.OZ = self.OY + self.lines * self.ny
        self.OX = self.OZ + 10 * self.xc
        self.RC = up8(self.OX + 10 * self.own)
        self.OM = up8(n * 5 * self.own)
        self.RA = 5 * self.H
        self.OFX = self.lat
        self.RF = up8(self.lat + 10 * self.own)
        self.OXQ = 5 * self.xc * self.R
        self.RK = up8(self.OXQ + 10 * self.zcl)
        self.RM = 5 * self.R + 8
        self.RP = self.OM + self.RM


def parts(x, count):
    out = []
    for _ in range(count):
        piece = x.astype(jnp.bfloat16)
        out.append(piece)
        x = x - piece.astype(jnp.float32)
    return out


def select_dot(pick, x, count=3, dims=(((1,), (0,)), ((), ()))):
    total = None
    for piece in parts(x, count):
        term = lax.dot_general(pick, piece, dims, preferred_element_type=jnp.float32)
        total = term if total is None else total + term
    return total


def lanes_at(x, index):
    return jnp.take_along_axis(x, index, axis=1, mode="promise_in_bounds")


def derived(U):
    inverse = 1.0 / U[0]
    velocity = [U[1] * inverse, U[2] * inverse, U[3] * inverse]
    kinetic = U[1] * velocity[0] + U[2] * velocity[1] + U[3] * velocity[2]
    pressure = (heat_ratio - 1.0) * (U[4] - 0.5 * kinetic)
    sound = jnp.sqrt(heat_ratio * pressure * inverse)
    return velocity, pressure, sound


def directed(U, speed, pressure, d):
    out = [U[0] * speed if d is None else U[1 + d]]
    out += [U[1 + e] * speed + (pressure if e == d else 0.0) if e == d else U[1 + e] * speed for e in range(3)]
    out.append((U[4] + pressure) * speed)
    return out


def twice_flux(L, dl, R, dr, d):
    fl = directed(L, dl[0], dl[1], d)
    fr = directed(R, dr[0], dr[1], d)
    signal = jnp.maximum(jnp.abs(dl[0]) + dl[2], jnp.abs(dr[0]) + dr[2])
    return [fl[v] + fr[v] - signal * (R[v] - L[v]) for v in range(5)]


def state_flux(L, R, d):
    vl, pl_, cl = derived(L)
    vr, pr, cr = derived(R)
    return twice_flux(L, (vl[d], pl_, cl), R, (vr[d], pr, cr), d)


def positions(z, ids, columns):
    down = lax.broadcasted_iota(jnp.int32, (z.S, z.S), 0)
    across = lax.broadcasted_iota(jnp.int32, (z.S, z.S), 1)
    number_row = ids[...].astype(jnp.float32)
    held = down.astype(jnp.float32) == number_row
    place = columns[...].astype(jnp.float32)
    rows = [jnp.sum(jnp.where(held, place[:, k : k + 1], 0.0), axis=0, keepdims=True) for k in range(2)]
    turn = lambda r: jnp.sum(jnp.where(down == across, r, 0.0), axis=1, keepdims=True)
    whole = lambda a: a.astype(jnp.int32)
    return turn(number_row), whole(turn(rows[0])), whole(turn(rows[1])), whole(rows[0]), whole(rows[1])


def extract_kernel(z, fine, coarse, com, scr):
    lane = lax.broadcasted_iota(jnp.int32, (z.P, LANES), 1)
    pick = z.P * ((lane % z.P) % z.zg) + jnp.where(lane >= 3 * z.P, z.P - 1, 0)
    group = jnp.where(lane >= 2 * z.P, (lane % z.P) // z.zg, -1)
    for q in range(z.own):
        for v in range(5):
            first = fine[v, q, :, :LANES]
            last = fine[v, q, :, (z.G - 1) * LANES :]
            face = jnp.where(lane < z.P, first, pltpu.roll(last, 2 * z.P, 1))
            for g in range(z.G):
                chunk = fine[v, q, :, g * LANES : (g + 1) * LANES]
                face = jnp.where(group == g, lanes_at(chunk, pick), face)
            scr[v % 2] = face
            for a in range(z.xa):
                com[pl.ds((v * z.xa + a) * z.own + q, z.n, stride=z.RC), :] = scr[v % 2, pl.ds(a, z.n, stride=z.xa), :]
            for side in range(2):
                row = fine[v, q, side * (z.P - 1) : side * (z.P - 1) + 1, :]
                place = z.OX + (side * 5 + v) * z.own + q
                for j in range(z.n):
                    com[j * z.RC + place : j * z.RC + place + 1, : z.PL] = row[:, j * z.PL : (j + 1) * z.PL]
    line = lax.broadcasted_iota(jnp.int32, (z.lines, LANES), 0)
    at = lax.broadcasted_iota(jnp.int32, (z.lines, LANES), 1)
    chosen = (at == z.H * (line // 2) + (z.H - 1) * (line % 2)).astype(jnp.bfloat16)
    width = 5 * z.xc * z.R
    for j in range(z.n):
        block = coarse[:, j * z.xc : (j + 1) * z.xc].reshape(width, LANES)
        lines = select_dot(chosen, block, 3, (((1,), (1,)), ((), ())))
        for t in range(z.ny):
            extent = min(LANES, width - t * LANES)
            com[j * z.RC + z.OY + t * z.lines : j * z.RC + z.OY + (t + 1) * z.lines, :extent] = lines[
                :, t * LANES : t * LANES + extent
            ]
        for v in range(5):
            for x in range(z.xc):
                row = j * z.RC + z.OZ + (v * z.xc + x) * 2
                com[row : row + 1, :] = coarse[v, j * z.xc + x, 0:1, :]
                com[row + 1 : row + 2, :] = coarse[v, j * z.xc + x, z.R - 1 : z.R, :]


def pack_kernel(z, com, outer, ids, up, dn):
    for side, margin in ((1, up), (0, dn)):
        for i in range(z.n):
            k = i * z.RC + z.OX + side * 5 * z.own
            margin[i * 5 * z.own : (i + 1) * 5 * z.own, :] = com[k : k + 5 * z.own, :]
        for v in range(5):
            margin[z.OM + v * z.R : z.OM + (v + 1) * z.R, :] = outer[v, side]
        margin[z.OM + 5 * z.R : z.OM + 5 * z.R + 8, :] = jnp.zeros((8, LANES), jnp.float32)
        margin[z.OM + 5 * z.R : z.OM + 5 * z.R + 1, : z.S] = ids[...].astype(jnp.float32)


def advance_kernel(z, fine, updated, avg, work, xflux, zflux, sums):
    count = z.own
    patch = pl.program_id(0)
    X = min(XROWS, z.P)
    lane = lax.broadcasted_iota(jnp.int32, (X, LANES), 1)
    row = lax.broadcasted_iota(jnp.int32, (X, LANES), 0)
    inner_y = lane % z.P < z.P - 1
    first_z = lane < z.P

    def first_pass(i, carry):
        at = pl.ds(pl.multiple_of(i * LANES, LANES), LANES)
        U = [fine[v, 0, :, at] for v in range(5)]
        velocity, pressure, sound = derived(U)
        for k, value in enumerate(U + velocity + [pressure, sound]):
            work[k, i, : z.P, :] = value
        return carry

    lax.fori_loop(0, z.G, first_pass, 0)
    xflux[:, :8, :] = jnp.zeros((5, 8, LANES), jnp.float32)

    def second_pass(i, carry):
        at = pl.ds(pl.multiple_of(i * LANES, LANES), LANES)
        nxt = jnp.minimum(i + 1, z.G - 1)
        inner_z = jnp.logical_or(lane < LANES - z.P, i < z.G - 1)
        for r in range(0, z.P, X):
            rows = slice(r, r + X)
            U = [work[k, i, rows, :] for k in range(5)]
            D = [work[k, i, rows, :] for k in range(5, 10)]
            XU = [work[k, i, r + 1 : r + 1 + X, :] for k in range(5)]
            XD = [work[k, i, r + 1 : r + 1 + X, :] for k in (5, 8, 9)]
            F = twice_flux(U, (D[0], D[3], D[4]), XU, XD, 0)
            change = []
            for v in range(5):
                face = jnp.where(row < z.P - 1 - r, F[v], 0.0) if r + X == z.P else F[v]
                xflux[v, 8 + r : 8 + r + X, :] = face
                change.append(face - xflux[v, 7 + r : 7 + r + X, :])
            ahead = lambda a: pltpu.roll(a, LANES - 1, 1)
            F = twice_flux(U, (D[1], D[3], D[4]), [ahead(a) for a in U], [ahead(D[k]) for k in (1, 3, 4)], 1)
            for v in range(5):
                face = jnp.where(inner_y, F[v], 0.0)
                change[v] = change[v] + (face - pltpu.roll(face, 1, 1))
            beyond = lambda k, a: pltpu.roll(jnp.where(first_z, work[k, nxt, rows, :], a), LANES - z.P, 1)
            F = twice_flux(
                U,
                (D[2], D[3], D[4]),
                [beyond(k, U[k]) for k in range(5)],
                [beyond(5 + k, D[k]) for k in (2, 3, 4)],
                2,
            )
            for v in range(5):
                face = jnp.where(inner_z, F[v], 0.0)
                rolled = pltpu.roll(face, z.P, 1)
                before = jnp.where(i == 0, 0.0, zflux[v, rows, :])
                zflux[v, rows, :] = rolled
                new = U[v] - (0.5 * fine_rate) * (change[v] + (face - jnp.where(first_z, before, rolled)))
                updated[v, patch, rows, at] = new
                sums[v, patch * z.G + i, rows, :] = new
        return carry

    lax.fori_loop(0, z.G, second_pass, 0)

    @pl.when(patch == count - 1)
    def _():
        half = z.zg // 2
        depth = z.xc * count * LANES
        source = lax.broadcasted_iota(jnp.int32, (depth, half * LANES), 0)
        target = lax.broadcasted_iota(jnp.int32, (depth, half * LANES), 1)
        place = source % LANES
        piece = source // LANES
        mean = (
            (piece == (target % LANES) // z.H)
            & (place // (2 * z.P) == target // LANES)
            & ((place % z.P) // 2 == target % z.H)
        )
        mean = jnp.where(mean, 0.125, 0.0).astype(jnp.bfloat16)

        def average(v, carry):
            columns = []
            for x in range(z.xc):
                for q in range(count):
                    blocks = []
                    for g in range(z.G):
                        i = q * z.G + g
                        blocks.append(
                            sums[v, i, pl.ds(2 * x, z.n, stride=z.xa), :] + sums[v, i, pl.ds(2 * x + 1, z.n, stride=z.xa), :]
                        )
                    columns.append(jnp.concatenate(blocks, axis=0))
            lhs = jnp.concatenate(parts(jnp.concatenate(columns, axis=1), 3), axis=0)
            got = jnp.dot(lhs, mean, preferred_element_type=jnp.float32)
            lines = z.G * z.n
            got = got[:lines] + got[lines : 2 * lines] + got[2 * lines :]
            for g in range(z.G):
                for h in range(half):
                    rows = pl.ds(v * z.H + half * g + h, z.n, stride=z.RA)
                    value = got[g * z.n : (g + 1) * z.n, h * LANES : (h + 1) * LANES]
                    avg[rows, :] = value
            return carry

        lax.fori_loop(0, 5, average, 0)


def provisional_kernel(z, columns, coarse, out, bare, outer, pad):
    rank = lax.axis_index("patch")
    row = lax.broadcasted_iota(jnp.int32, (z.R, LANES), 0)
    lane = lax.broadcasted_iota(jnp.int32, (z.R, LANES), 1)
    S = columns.shape[0]
    gy = columns[:, 0:1]
    turn = lax.broadcasted_iota(jnp.int32, (S, S), 0) == lax.broadcasted_iota(jnp.int32, (S, S), 1)
    gzr = jnp.sum(jnp.where(turn, columns[:, 1:2].astype(jnp.float32), 0.0), axis=0, keepdims=True).astype(jnp.int32)
    block = lambda a: (a + z.H) // z.H - 1
    place = lax.broadcasted_iota(jnp.int32, (z.R, S), 0) + rank * z.R
    across = lax.broadcasted_iota(jnp.int32, (S, LANES), 1)

    def uncovered(dz, dy):
        rows = (block(place + dz) == gzr + 1).astype(jnp.bfloat16)
        lanes = (block(across + dy) == gy + 1).astype(jnp.bfloat16)
        return 1.0 - jnp.dot(rows, lanes, preferred_element_type=jnp.float32)

    own, zu, zd, yu, yd = [uncovered(*shift) for shift in ((0, 0), (1, 0), (-1, 0), (0, 1), (0, -1))]
    zu = jnp.where(row < z.R - 1, zu, 0.0)
    zd = jnp.where(row > 0, zd, 0.0)
    bare[...] = own
    for v in range(5):
        outer[v, 0] = coarse[v, 0]
        outer[v, 1] = coarse[v, z.NX - 1]

    def layer(x, carry):
        U = [coarse[v, x] for v in range(5)]
        vel, pressure, sound = derived(U)
        last = jnp.minimum(x + 1, z.NX - 1)
        XU = [coarse[v, last] for v in range(5)]
        xvel, xp, xs = derived(XU)
        fx = twice_flux(U, (vel[0], pressure, sound), XU, (xvel[0], xp, xs), 0)
        inner = jnp.where(x < z.NX - 1, 1.0, 0.0)
        D = [vel[1], pressure, sound]
        move = lambda a: jnp.where(lane == LANES - 1, a, pltpu.roll(a, LANES - 1, 1))
        fy = twice_flux(U, D, [move(a) for a in U], [move(a) for a in D], 1)
        edge = twice_flux(U, D, U, D, 1)
        D = [vel[2], pressure, sound]
        move = lambda a: pltpu.roll(a, z.R - 1, 0)
        fz = twice_flux(U, D, [move(a) for a in U], [move(a) for a in D], 2)
        for v in range(5):
            face = fx[v] * inner
            below = jnp.where(x == 0, 0.0, pad[v])
            pad[v] = face
            ylow = jnp.where(lane == 0, edge[v], pltpu.roll(fy[v], 1, 1))
            zlow = pltpu.roll(fz[v], 1, 0)
            total = face - below + (fy[v] * yu - ylow * yd) + (fz[v] * zu - zlow * zd)
            out[v, x] = jnp.where(own > 0.0, U[v] - (0.5 * coarse_rate) * total, 0.0)
        return carry

    lax.fori_loop(0, z.NX, layer, 0)


def side_kernel(z, ids, columns, com, ghost, lat):
    S, f_of = z.S, z.P
    _, gy, gz, gyr, gzr = positions(z, ids, columns)
    lane = lax.broadcasted_iota(jnp.int32, (S, LANES), 1)
    kind = lane // f_of
    even = kind % 2 == 0
    steps = ((0, -1), (0, 1), (-1, 0), (1, 0))
    flags = [((gyr == gy + dy) & (gzr == gz + dz)).astype(jnp.float32) for dy, dz in steps]
    here = jnp.zeros((S, LANES), jnp.float32)
    for k in range(4):
        here = jnp.where(kind == k, jnp.sum(flags[k], axis=1, keepdims=True), here)
    picks = jnp.concatenate(flags, axis=1).astype(jnp.bfloat16)

    for i in range(z.n):
        for k in range(5 * z.xa):
            lat[k * S + i * z.own : k * S + (i + 1) * z.own, :] = com[i * z.RC + k * z.own : i * z.RC + (k + 1) * z.own, :]

    def onehot(index, extent):
        return (lax.broadcasted_iota(jnp.int32, (S, extent), 1) == index).astype(jnp.bfloat16)

    vx = 5 * z.xc
    low_lines = jnp.concatenate([com[pl.ds(z.OZ + 2 * k + 1, z.n, stride=z.RC), :] for k in range(vx)], axis=1)
    top_lines = jnp.concatenate([com[pl.ds(z.OZ + 2 * k, z.n, stride=z.RC), :] for k in range(vx)], axis=1)
    low_rows = select_dot(onehot(gz * z.m + z.m - 1, z.n), low_lines)
    top_rows = select_dot(onehot((gz + 2) * z.m, z.n), top_lines)
    y_index = z.H * (gy + 1) + (lane % f_of) // 2
    half = (lane % f_of) // 2
    y_rows = {}
    for t in range(z.ny):
        table = jnp.concatenate(
            [com[i * z.RC + z.OY + t * z.lines : i * z.RC + z.OY + (t + 1) * z.lines, :] for i in range(z.n)], axis=0
        )
        for h in range(z.m):
            for f, line in ((2, 2 * gy + 1), (3, 2 * (gy + 2))):
                y_rows[t, h, f] = select_dot(onehot(((gz + 1) * z.m + h) * z.lines + line, z.n * z.lines), table)
    for v in range(5):
        swapped = []
        for a in range(z.xa):
            T = lat[(v * z.xa + a) * S : (v * z.xa + a + 1) * S, :]
            T = jnp.where(even, pltpu.roll(T, LANES - f_of, 1), pltpu.roll(T, f_of, 1))
            swapped.append(jnp.concatenate([jnp.where(kind == k, T, 0.0) for k in range(4)], axis=0))
        near = select_dot(picks, jnp.concatenate(swapped, axis=1))
        for x in range(z.xc):
            k = v * z.xc + x
            at = slice(k * LANES, (k + 1) * LANES)
            c = jnp.where(kind == 0, lanes_at(low_rows[:, at], y_index), lanes_at(top_rows[:, at], y_index))
            start = k * z.R
            for f in (2, 3):
                for h in range(z.m):
                    got = lanes_at(y_rows[start // LANES, h, f], start % LANES + half % z.R)
                    c = jnp.where((kind == f) & (half // z.R == h), got, c)
            for a in (2 * x, 2 * x + 1):
                ghost[(v * z.xa + a) * S : (v * z.xa + a + 1) * S, :] = jnp.where(
                    here > 0.0, near[:, a * LANES : (a + 1) * LANES], c
                )

    is_z = kind < 2
    sign = jnp.where(even, 0.5 * fine_rate, -0.5 * fine_rate)
    for a in range(z.xa):
        at = [slice((v * z.xa + a) * S, (v * z.xa + a + 1) * S) for v in range(5)]
        own = [lat[s, :] for s in at]
        far = [ghost[s, :] for s in at]
        L = [jnp.where(even, far[v], own[v]) for v in range(5)]
        R = [jnp.where(even, own[v], far[v]) for v in range(5)]
        vl, pl_, cl = derived(L)
        vr, pr, cr = derived(R)
        sl = jnp.where(is_z, vl[2], vl[1])
        sr = jnp.where(is_z, vr[2], vr[1])
        F = twice_flux(L, (sl, pl_, cl), R, (sr, pr, cr), None)
        both = pl_ + pr
        F[2] = F[2] + jnp.where(is_z, 0.0, both)
        F[3] = F[3] + jnp.where(is_z, both, 0.0)
        for v in range(5):
            C = sign * F[v]
            ghost[at[v], :] = C


def end_kernel(z, ids, columns, com, ghost, below, above, outf, xc, xs):
    S = z.S
    slab = lax.axis_index("slab")
    number = positions(z, ids, columns)[0]
    for d in range(z.n):
        for k in range(5 * z.xa):
            outf[d * z.RF + k * z.own : d * z.RF + (k + 1) * z.own, :] = ghost[k * S + d * z.own : k * S + (d + 1) * z.own, :]
    for w, (source, pitch, offset) in enumerate(
        ((com, z.RC, z.OX), (com, z.RC, z.OX + 5 * z.own), (below, 5 * z.own, 0), (above, 5 * z.own, 0))
    ):
        for i in range(z.n):
            for v in range(5):
                k = (w * 5 + v) * S + i * z.own
                r = i * pitch + offset + v * z.own
                xs[k : k + z.own, :] = source[r : r + z.own, :]
    for side, (margin, edge) in enumerate(((below, slab == 0), (above, slab == z.slabs - 1))):
        match = (number == margin[z.OM + 5 * z.R : z.OM + 5 * z.R + 1, :S]).astype(jnp.bfloat16)
        own = [xs[(side * 5 + v) * S : (side * 5 + v + 1) * S, :] for v in range(5)]
        far = select_dot(
            match, jnp.concatenate([xs[((2 + side) * 5 + v) * S : ((2 + side) * 5 + v + 1) * S, :] for v in range(5)], axis=1)
        )
        far = [jnp.where(edge, own[v], far[:, v * LANES : (v + 1) * LANES]) for v in range(5)]
        F = state_flux(far, own, 0) if side == 0 else state_flux(own, far, 0)
        for v in range(5):
            C = (0.5 * fine_rate if side == 0 else -0.5 * fine_rate) * F[v]
            xc[(side * 5 + v) * S : (side * 5 + v + 1) * S, :] = C
            for d in range(z.n):
                k = d * z.RF + z.OFX + (side * 5 + v) * z.own
                outf[k : k + z.own, :] = C[d * z.own : (d + 1) * z.own]


def canvas_kernel(z, ids_s, columns_s, ids, columns, com, ghost, xc, avg, *rest):
    outs, (canvas, ends) = rest[: z.n], rest[z.n :]
    S, f_of = z.S, z.P
    vx = 5 * z.xc
    _, gy, gz, gyr, gzr = positions(z, ids, columns)
    lane = lax.broadcasted_iota(jnp.int32, (S, LANES), 1)
    steps = ((0, -1), (0, 1), (-1, 0), (1, 0))
    flags = [((gyr == gy + dy) & (gzr == gz + dz)).astype(jnp.float32) for dy, dz in steps]
    turned = [((gy == gyr + dy) & (gz == gzr + dz)).astype(jnp.float32) for dy, dz in steps]
    absent_row = [1.0 - jnp.sum(t, axis=0, keepdims=True) for t in turned]
    zrow = lax.broadcasted_iota(jnp.int32, (z.NZ, S), 0)
    base = z.H * (gzr + 1)
    zmat = jnp.concatenate(
        [
            (zrow == base).astype(jnp.float32) - absent_row[0] * (zrow == base - 1).astype(jnp.float32),
            (zrow == base + z.H - 1).astype(jnp.float32) - absent_row[1] * (zrow == base + z.H).astype(jnp.float32),
        ],
        axis=1,
    ).astype(jnp.bfloat16)
    ybase = z.H * (gy + 1)
    absent = [1.0 - jnp.sum(flags[k], axis=1, keepdims=True) for k in (2, 3)]
    ymat = jnp.concatenate(
        [
            (lane == ybase).astype(jnp.float32) - absent[0] * (lane == ybase - 1).astype(jnp.float32),
            (lane == ybase + z.H - 1).astype(jnp.float32) - absent[1] * (lane == ybase + z.H).astype(jnp.float32),
        ],
        axis=0,
    ).astype(jnp.bfloat16)
    in_y = lane // z.H == gy + 1
    in_z = lane // z.H == gz + 1
    zq, yq = [], []
    for v in range(5):
        for x in range(z.xc):
            r = (v * z.xa + 2 * x) * S
            Q = ghost[r : r + S, :] + ghost[r + S : r + 2 * S, :]
            Q = 0.125 * (Q + pltpu.roll(Q, LANES - 1, 1))
            got = [lanes_at(Q, f_of * f + 2 * (lane % z.H)) for f in range(4)]
            zq.append(jnp.concatenate([jnp.where(in_y, got[f], 0.0) for f in (0, 1)], axis=0))
            yq.append(jnp.concatenate([jnp.where(in_z, got[f], 0.0) for f in (2, 3)], axis=0))
    zsum = select_dot(zmat, jnp.concatenate(zq, axis=1), 2)
    ysum = None
    for piece in parts(jnp.concatenate([a.T for a in yq], axis=0), 2):
        term = jnp.dot(piece, ymat, preferred_element_type=jnp.float32)
        ysum = term if ysum is None else ysum + term
    for k in range(vx):
        canvas[k * z.NZ : (k + 1) * z.NZ, :] = zsum[:, k * LANES : (k + 1) * LANES] + ysum[k * z.NZ : (k + 1) * z.NZ, :]
    rank = lax.broadcasted_iota(jnp.int32, (z.n, LANES), 0)
    rank_slot = lax.broadcasted_iota(jnp.int32, (z.n, S), 0)
    inside_y = in_y.astype(jnp.bfloat16)
    cover = lambda block: jnp.dot((block == gzr + 1).astype(jnp.bfloat16), inside_y, preferred_element_type=jnp.float32)
    bare_first = 1.0 - cover((rank_slot * z.R) // z.H)
    bare_last = 1.0 - cover((rank_slot * z.R + z.R - 1) // z.H)
    low_mask = bare_first * jnp.where(rank == 0, 1.0, pltpu.roll(bare_last, 1, 0))
    top_mask = bare_last * jnp.where(rank == z.n - 1, 1.0, pltpu.roll(bare_first, z.n - 1, 0))
    for x in range(z.xc):
        lines = [[com[pl.ds(z.OZ + 2 * (v * z.xc + x) + s, z.n, stride=z.RC), :] for v in range(5)] for s in (0, 1)]
        under = [jnp.where(rank == 0, lines[0][v], pltpu.roll(lines[1][v], 1, 0)) for v in range(5)]
        over = [jnp.where(rank == z.n - 1, lines[1][v], pltpu.roll(lines[0][v], z.n - 1, 0)) for v in range(5)]
        low = state_flux(under, lines[0], 2)
        top = state_flux(lines[1], over, 2)
        for v in range(5):
            first = pl.ds((v * z.xc + x) * z.NZ, z.n, stride=z.R)
            last = pl.ds((v * z.xc + x) * z.NZ + z.R - 1, z.n, stride=z.R)
            canvas[first, :] = canvas[first, :] + (0.5 * coarse_rate) * low_mask * low[v]
            canvas[last, :] = canvas[last, :] - (0.5 * coarse_rate) * top_mask * top[v]

    spot = lax.broadcasted_iota(jnp.int32, (z.H, LANES), 1) // z.H

    def place(k, carry):
        i = k // z.own
        q = k % z.own
        sy = columns_s[ids_s[0, k], 0] + 1
        sz = columns_s[ids_s[0, k], 1] + 1
        inside = spot == sy
        for v in range(5):
            block = avg[pl.ds(pl.multiple_of(i * z.RA + v * z.H, 8), z.H), :]
            for x in range(z.xc):
                shift = lax.rem(z.H * (sy - (x * z.own + q)) + 2 * LANES, LANES)
                rows = pl.ds(pl.multiple_of((v * z.xc + x) * z.NZ + z.H * sz, z.H), z.H)
                canvas[rows, :] = canvas[rows, :] + jnp.where(inside, pltpu.roll(block, shift, 1), 0.0)
        return carry

    lax.fori_loop(0, S, place, 0, unroll=4)
    zb = (rank_slot // z.m == gzr + 1).astype(jnp.bfloat16)
    tops = []
    for side in range(2):
        for v in range(5):
            C = xc[(side * 5 + v) * S : (side * 5 + v + 1) * S, :]
            Q = C + pltpu.roll(C, LANES - 1, 1)
            Q = 0.125 * (Q + pltpu.roll(Q, LANES - z.P, 1))
            for h in range(z.zcl):
                tops.append(jnp.where(in_y, lanes_at(Q, 2 * z.P * h + 2 * (lane % z.H)), 0.0))
    tops = select_dot(zb, jnp.concatenate(tops, axis=1), 2)
    for e in range(10 * z.zcl):
        ends[e] = tops[:, e * LANES : (e + 1) * LANES]
    rank = lax.axis_index("patch")
    for k, out in enumerate(outs):
        d = lax.rem(rank + k, z.n)
        for e in range(vx):
            out[e * z.R : (e + 1) * z.R, :] = canvas[pl.ds(pl.multiple_of(e * z.NZ + d * z.R, 8), z.R), :]
        for e in range(10 * z.zcl):
            out[z.OXQ + e : z.OXQ + e + 1, :] = ends[e, pl.ds(d, 1), :]


def fine_kernel(z, updated, recv, out, scr):
    q = pl.program_id(0)
    lane = lax.broadcasted_iota(jnp.int32, (z.P, LANES), 1)
    y = lane % z.P
    edge = (y == 0) | (y == z.P - 1)
    pick = jnp.where(y == 0, 2 * z.P, 3 * z.P) + lane // z.P
    for v in range(5):
        for a in range(z.xa):
            scr[v % 2, pl.ds(a, z.n, stride=z.xa), :] = recv[pl.ds((v * z.xa + a) * z.own + q, z.n, stride=z.RF), :]
        face = scr[v % 2]
        for g in range(z.G):
            at = slice(g * LANES, (g + 1) * LANES)
            add = jnp.where(edge, lanes_at(face, jnp.where(edge, pick + z.zg * g, 0)), 0.0)
            if g == 0:
                add = add + jnp.where(lane < z.P, face, 0.0)
            if g == z.G - 1:
                add = add + jnp.where(lane >= LANES - z.P, pltpu.roll(face, 2 * z.P, 1), 0.0)
            out[v, 0, :, at] = updated[v, q, :, at] + add
        for side in range(2):
            x = side * (z.P - 1)
            for j in range(z.n):
                r = j * z.RF + z.OFX + (side * 5 + v) * z.own + q
                at = slice(j * z.PL, (j + 1) * z.PL)
                out[v, 0, x : x + 1, at] = out[v, 0, x : x + 1, at] + recv[pl.ds(r, 1), : z.PL]


def coarse_kernel(z, prov, bare, coarse, below, above, *rest):
    recv, out = rest[: z.n], rest[z.n]
    slab, rank = lax.axis_index("slab"), lax.axis_index("patch")
    offset = lax.rem(rank, z.m) * z.R
    for k in range(z.n):
        j = lax.rem(rank + z.n - k, z.n)
        for v in range(5):
            for x in range(z.xc):
                r = (v * z.xc + x) * z.R
                out[v, j * z.xc + x] = prov[v, j * z.xc + x] + recv[k][r : r + z.R, :]
    for side, margin, edge in ((0, below, slab == 0), (1, above, slab == z.slabs - 1)):
        x = side * (z.NX - 1)
        own = [coarse[v, side] for v in range(5)]
        far = [jnp.where(edge, own[v], margin[z.OM + v * z.R : z.OM + (v + 1) * z.R, :]) for v in range(5)]
        F = state_flux(far, own, 0) if side == 0 else state_flux(own, far, 0)
        scale = (0.5 if side == 0 else -0.5) * coarse_rate * bare[...]
        for v in range(5):
            out[v, x] = out[v, x] + scale * F[v]
    for k in range(z.n):
        j = lax.rem(rank + z.n - k, z.n)
        for h in range(z.zcl):
            row = j * z.zcl + h - offset
            inside = (row >= 0) & (row < z.R)
            row = jnp.clip(row, 0, z.R - 1)
            for v in range(5):
                for side in range(2):
                    x = side * (z.NX - 1)
                    r = z.OXQ + (side * 5 + v) * z.zcl + h
                    add = jnp.where(inside, recv[k][r : r + 1, :], 0.0)
                    out[v, x, pl.ds(row, 1), :] = out[v, x, pl.ds(row, 1), :] + add


def held(a):
    return pltpu.with_memory_space_constraint(a, pltpu.VMEM)


def call(kernel, z, outs, ins, scratch=(), keep=True):
    return pl.pallas_call(
        functools.partial(kernel, z),
        out_shape=[pltpu.VMEM(s, jnp.float32) if keep else jax.ShapeDtypeStruct(s, jnp.float32) for s in outs],
        in_specs=[SMEM if space == "s" else VMEM for space, _ in ins],
        out_specs=[VMEM] * len(outs),
        scratch_shapes=[pltpu.VMEM(s, jnp.float32) for s in scratch],
        compiler_params=pltpu.CompilerParams(vmem_limit_bytes=VMEM_LIMIT),
    )(*[held(a) if space == "p" else a for space, a in ins])


def run_advance(z, fine):
    block = pl.BlockSpec((5, 1) + fine.shape[2:], lambda i: (0, i, 0, 0))
    average = (z.n * z.RA, LANES)
    return pl.pallas_call(
        functools.partial(advance_kernel, z),
        grid=(z.own,),
        out_shape=[pltpu.VMEM(fine.shape, jnp.float32), pltpu.VMEM(average, jnp.float32)],
        in_specs=[block],
        out_specs=[VMEM, VMEM],
        scratch_shapes=[
            pltpu.VMEM(s, jnp.float32)
            for s in ((10, z.G, z.P + 8, LANES), (5, z.P + 8, LANES), (5, z.P, LANES), (5, z.own * z.G, z.P, LANES))
        ],
        compiler_params=pltpu.CompilerParams(vmem_limit_bytes=VMEM_LIMIT),
        name="advance",
    )(fine)


def run_fine(z, updated, recv):
    block = pl.BlockSpec((5, 1) + updated.shape[2:], lambda i: (0, i, 0, 0))
    return pl.pallas_call(
        functools.partial(fine_kernel, z),
        grid=(z.own,),
        out_shape=jax.ShapeDtypeStruct(updated.shape, jnp.float32),
        in_specs=[VMEM, VMEM],
        out_specs=block,
        scratch_shapes=[pltpu.VMEM((2, z.P, LANES), jnp.float32)],
        compiler_params=pltpu.CompilerParams(vmem_limit_bytes=VMEM_LIMIT),
        name="fine_edges",
    )(held(updated), held(recv))


def local(n, slabs, coarse, fine, columns, patch_ids):
    return level_step(n, slabs, coarse, fine, columns, patch_ids)


def level_step(n, slabs, coarse, fine, columns, patch_ids):
    slots = patch_ids.shape[1]
    assert columns.shape[0] == slots
    z = Sizes(n, slabs, fine.shape, coarse.shape, slots)

    def exchange(a):
        return lax.all_to_all(a, "patch", 0, 0, tiled=True)

    def shifted(a, step):
        pairs = [(i, i + step) for i in range(slabs) if 0 <= i + step < slabs]
        return lax.ppermute(a, "slab", pairs)

    faces = (5 * z.xa * slots, LANES)
    (com,) = call(extract_kernel, z, [(n * z.RC, LANES)], [("v", fine), ("v", coarse)], [(2, z.P, LANES)])
    com = exchange(com)
    updated, avg = run_advance(z, fine)
    avg = exchange(avg)
    prov, bare, outer = call(
        provisional_kernel,
        z,
        [coarse.shape, (z.R, LANES), (5, 2, z.R, LANES)],
        [("v", columns), ("v", coarse)],
        [(5, z.R, LANES)],
    )
    up, dn = call(pack_kernel, z, [(z.RP, LANES)] * 2, [("p", com), ("p", outer), ("v", patch_ids)])
    below = shifted(up, 1)
    above = shifted(dn, -1)
    (ghost,) = call(side_kernel, z, [faces], [("v", patch_ids), ("v", columns), ("p", com)], [faces])
    outf, xc = call(
        end_kernel,
        z,
        [(n * z.RF, LANES), (10 * slots, LANES)],
        [("v", patch_ids), ("v", columns)] + [("p", a) for a in (com, ghost, below, above)],
        [(20 * slots, LANES)],
    )
    outf = exchange(outf)
    pieces = list(call(
        canvas_kernel,
        z,
        [(z.RK, LANES)] * n,
        [("s", patch_ids), ("s", columns), ("v", patch_ids), ("v", columns)]
        + [("p", a) for a in (com, ghost, xc, avg)],
        [(5 * z.xc * z.NZ, LANES), (10 * z.zcl, n, LANES)],
    ))
    for k in range(1, n):
        pieces[k] = lax.ppermute(pieces[k], "patch", [(i, (i + k) % n) for i in range(n)])
    fine_out = run_fine(z, updated, outf)
    (coarse_out,) = call(
        coarse_kernel, z, [coarse.shape], [("p", a) for a in (prov, bare, outer, below, above, *pieces)], keep=False
    )
    return coarse_out, fine_out


def solution(mesh):
    n, slabs = mesh.shape["patch"], mesh.shape["slab"]
    return jax.shard_map(
        functools.partial(local, n, slabs),
        mesh=mesh,
        in_specs=(
            P(None, "slab", "patch", None),
            P(None, ("slab", "patch"), None, None),
            P(),
            P("slab", None),
        ),
        out_specs=(P(None, "slab", "patch", None), P(None, ("slab", "patch"), None, None)),
        check_vma=False,
    )
```

```python
import functools

import jax
import jax.numpy as jnp
from jax import lax
from jax.experimental import pallas as pl
from jax.experimental.pallas import tpu as pltpu
from jax.sharding import PartitionSpec as P


LANES = 128
XROWS = 16
VMEM_LIMIT = 24 * 1024 * 1024
heat_ratio = 1.4
fine_rate = 0.1
coarse_rate = 0.05
VMEM = pl.BlockSpec(memory_space=pltpu.VMEM)
SMEM = pl.BlockSpec(memory_space=pltpu.SMEM)


def up8(count):
    return -(-count // 8) * 8


class Sizes:
    def __init__(self, n, slabs, fine_shape, coarse_shape, slots):
        self.n, self.slabs, self.S = n, slabs, slots
        self.own = fine_shape[1]
        self.P = fine_shape[2]
        self.cells = fine_shape[3]
        self.H = self.P // 2
        self.G = self.cells // LANES
        self.zg = LANES // self.P
        self.xa = self.P // n
        self.xc = self.H // n
        self.PL = self.cells // n
        self.zcl = self.P // n // 2
        self.NX, self.R, self.NY = coarse_shape[1:]
        self.m = self.H // self.R
        self.NZ = self.R * n
        self.lines = 2 * (self.NY // self.H)
        assert self.NX == self.H and self.NY == LANES and self.H % self.R == 0
        assert self.P % (2 * n) == 0 and 4 * self.P == LANES and slots == self.own * n
        self.lat = 5 * self.xa * self.own
        self.width = 5 * self.xc * self.R
        self.tail = max(self.width - LANES, 0)
        assert 4 * self.tail in (0, LANES)
        self.OY = up8(self.lat)
        self.OT = self.OY + self.lines
        self.OZ = self.OT + (self.lines // 4 if self.tail else 0)
        self.OX = self.OZ + 10 * self.xc
        self.RC = up8(self.OX + 10 * self.own)
        self.OM = up8(n * 5 * self.own)
        self.RA = 5 * self.H
        self.OFX = self.lat
        self.RF = up8(self.lat + 10 * self.own)
        self.OXQ = 5 * self.xc * self.R
        self.RK = up8(self.OXQ + 10 * self.zcl)
        self.RM = 5 * self.R + 8
        self.RP = self.OM + self.RM


def parts(x, count):
    out = []
    for _ in range(count):
        piece = x.astype(jnp.bfloat16)
        out.append(piece)
        x = x - piece.astype(jnp.float32)
    return out


def select_dot(pick, x, count=3, dims=(((1,), (0,)), ((), ()))):
    total = None
    for piece in parts(x, count):
        term = lax.dot_general(pick, piece, dims, preferred_element_type=jnp.float32)
        total = term if total is None else total + term
    return total


def lanes_at(x, index):
    return jnp.take_along_axis(x, index, axis=1, mode="promise_in_bounds")


def derived(U):
    inverse = 1.0 / U[0]
    velocity = [U[1] * inverse, U[2] * inverse, U[3] * inverse]
    kinetic = U[1] * velocity[0] + U[2] * velocity[1] + U[3] * velocity[2]
    pressure = (heat_ratio - 1.0) * (U[4] - 0.5 * kinetic)
    sound = jnp.sqrt(heat_ratio * pressure * inverse)
    return velocity, pressure, sound


def directed(U, speed, pressure, d):
    out = [U[0] * speed if d is None else U[1 + d]]
    out += [U[1 + e] * speed + (pressure if e == d else 0.0) if e == d else U[1 + e] * speed for e in range(3)]
    out.append((U[4] + pressure) * speed)
    return out


def twice_flux(L, dl, R, dr, d):
    fl = directed(L, dl[0], dl[1], d)
    fr = directed(R, dr[0], dr[1], d)
    signal = jnp.maximum(jnp.abs(dl[0]) + dl[2], jnp.abs(dr[0]) + dr[2])
    return [fl[v] + fr[v] - signal * (R[v] - L[v]) for v in range(5)]


def state_flux(L, R, d):
    vl, pl_, cl = derived(L)
    vr, pr, cr = derived(R)
    return twice_flux(L, (vl[d], pl_, cl), R, (vr[d], pr, cr), d)


def positions(z, ids, columns):
    down = lax.broadcasted_iota(jnp.int32, (z.S, z.S), 0)
    across = lax.broadcasted_iota(jnp.int32, (z.S, z.S), 1)
    number_row = ids[...].astype(jnp.float32)
    held = down.astype(jnp.float32) == number_row
    place = columns[...].astype(jnp.float32)
    rows = [jnp.sum(jnp.where(held, place[:, k : k + 1], 0.0), axis=0, keepdims=True) for k in range(2)]
    turn = lambda r: jnp.sum(jnp.where(down == across, r, 0.0), axis=1, keepdims=True)
    whole = lambda a: a.astype(jnp.int32)
    return turn(number_row), whole(turn(rows[0])), whole(turn(rows[1])), whole(rows[0]), whole(rows[1])


def extract_kernel(z, fine, coarse, com, scr):
    lane = lax.broadcasted_iota(jnp.int32, (z.P, LANES), 1)
    pick = z.P * ((lane % z.P) % z.zg) + jnp.where(lane >= 3 * z.P, z.P - 1, 0)
    group = jnp.where(lane >= 2 * z.P, (lane % z.P) // z.zg, -1)
    for q in range(z.own):
        for v in range(5):
            first = fine[v, q, :, :LANES]
            last = fine[v, q, :, (z.G - 1) * LANES :]
            face = jnp.where(lane < z.P, first, pltpu.roll(last, 2 * z.P, 1))
            for g in range(z.G):
                chunk = fine[v, q, :, g * LANES : (g + 1) * LANES]
                face = jnp.where(group == g, lanes_at(chunk, pick), face)
            scr[v % 2] = face
            for a in range(z.xa):
                com[pl.ds((v * z.xa + a) * z.own + q, z.n, stride=z.RC), :] = scr[v % 2, pl.ds(a, z.n, stride=z.xa), :]
            for side in range(2):
                row = fine[v, q, side * (z.P - 1) : side * (z.P - 1) + 1, :]
                place = z.OX + (side * 5 + v) * z.own + q
                for j in range(z.n):
                    com[j * z.RC + place : j * z.RC + place + 1, : z.PL] = row[:, j * z.PL : (j + 1) * z.PL]
    line = lax.broadcasted_iota(jnp.int32, (z.lines, LANES), 0)
    at = lax.broadcasted_iota(jnp.int32, (z.lines, LANES), 1)
    chosen = (at == z.H * (line // 2) + (z.H - 1) * (line % 2)).astype(jnp.bfloat16)
    quarter = z.lines // 4
    target = lax.broadcasted_iota(jnp.int32, (quarter, LANES), 1) // (LANES // 4)
    for j in range(z.n):
        block = coarse[:, j * z.xc : (j + 1) * z.xc].reshape(z.width, LANES)
        if z.tail:
            block = jnp.concatenate([block, jnp.zeros((2 * LANES - z.width, LANES), jnp.float32)], axis=0)
        lines = select_dot(chosen, block, 3, (((1,), (1,)), ((), ())))
        extent = min(LANES, z.width)
        com[j * z.RC + z.OY : j * z.RC + z.OY + z.lines, :extent] = lines[:, :extent]
        if z.tail:
            packed = jnp.zeros((quarter, LANES), jnp.float32)
            for b in range(4):
                moved = pltpu.roll(lines[:, LANES:], b * z.tail, 1)[b * quarter : (b + 1) * quarter]
                packed = jnp.where(target == b, moved, packed)
            com[j * z.RC + z.OT : j * z.RC + z.OT + quarter, :] = packed
        for v in range(5):
            for x in range(z.xc):
                row = j * z.RC + z.OZ + (v * z.xc + x) * 2
                com[row : row + 1, :] = coarse[v, j * z.xc + x, 0:1, :]
                com[row + 1 : row + 2, :] = coarse[v, j * z.xc + x, z.R - 1 : z.R, :]


def pack_kernel(z, com, outer, ids, up, dn):
    for side, margin in ((1, up), (0, dn)):
        for i in range(z.n):
            k = i * z.RC + z.OX + side * 5 * z.own
            margin[i * 5 * z.own : (i + 1) * 5 * z.own, :] = com[k : k + 5 * z.own, :]
        for v in range(5):
            margin[z.OM + v * z.R : z.OM + (v + 1) * z.R, :] = outer[v, side]
        margin[z.OM + 5 * z.R : z.OM + 5 * z.R + 8, :] = jnp.zeros((8, LANES), jnp.float32)
        margin[z.OM + 5 * z.R : z.OM + 5 * z.R + 1, : z.S] = ids[...].astype(jnp.float32)


def advance_kernel(z, fine, updated, avg, work, xflux, zflux, sums):
    count = z.own
    patch = pl.program_id(0)
    X = min(XROWS, z.P)
    lane = lax.broadcasted_iota(jnp.int32, (X, LANES), 1)
    row = lax.broadcasted_iota(jnp.int32, (X, LANES), 0)
    inner_y = lane % z.P < z.P - 1
    first_z = lane < z.P

    def first_pass(i, carry):
        at = pl.ds(pl.multiple_of(i * LANES, LANES), LANES)
        U = [fine[v, 0, :, at] for v in range(5)]
        velocity, pressure, sound = derived(U)
        for k, value in enumerate(U + velocity + [pressure, sound]):
            work[k, i, : z.P, :] = value
        return carry

    lax.fori_loop(0, z.G, first_pass, 0)
    xflux[:, :8, :] = jnp.zeros((5, 8, LANES), jnp.float32)

    def second_pass(i, carry):
        at = pl.ds(pl.multiple_of(i * LANES, LANES), LANES)
        nxt = jnp.minimum(i + 1, z.G - 1)
        inner_z = jnp.logical_or(lane < LANES - z.P, i < z.G - 1)
        for r in range(0, z.P, X):
            rows = slice(r, r + X)
            U = [work[k, i, rows, :] for k in range(5)]
            D = [work[k, i, rows, :] for k in range(5, 10)]
            XU = [work[k, i, r + 1 : r + 1 + X, :] for k in range(5)]
            XD = [work[k, i, r + 1 : r + 1 + X, :] for k in (5, 8, 9)]
            F = twice_flux(U, (D[0], D[3], D[4]), XU, XD, 0)
            change = []
            for v in range(5):
                face = jnp.where(row < z.P - 1 - r, F[v], 0.0) if r + X == z.P else F[v]
                xflux[v, 8 + r : 8 + r + X, :] = face
                change.append(face - xflux[v, 7 + r : 7 + r + X, :])
            ahead = lambda a: pltpu.roll(a, LANES - 1, 1)
            F = twice_flux(U, (D[1], D[3], D[4]), [ahead(a) for a in U], [ahead(D[k]) for k in (1, 3, 4)], 1)
            for v in range(5):
                face = jnp.where(inner_y, F[v], 0.0)
                change[v] = change[v] + (face - pltpu.roll(face, 1, 1))
            beyond = lambda k, a: pltpu.roll(jnp.where(first_z, work[k, nxt, rows, :], a), LANES - z.P, 1)
            F = twice_flux(
                U,
                (D[2], D[3], D[4]),
                [beyond(k, U[k]) for k in range(5)],
                [beyond(5 + k, D[k]) for k in (2, 3, 4)],
                2,
            )
            for v in range(5):
                face = jnp.where(inner_z, F[v], 0.0)
                rolled = pltpu.roll(face, z.P, 1)
                before = jnp.where(i == 0, 0.0, zflux[v, rows, :])
                zflux[v, rows, :] = rolled
                new = U[v] - (0.5 * fine_rate) * (change[v] + (face - jnp.where(first_z, before, rolled)))
                updated[v, patch, rows, at] = new
                sums[v, patch * z.G + i, rows, :] = new
        return carry

    lax.fori_loop(0, z.G, second_pass, 0)

    @pl.when(patch == count - 1)
    def _():
        half = z.zg // 2
        depth = z.xc * count * LANES
        source = lax.broadcasted_iota(jnp.int32, (depth, half * LANES), 0)
        target = lax.broadcasted_iota(jnp.int32, (depth, half * LANES), 1)
        place = source % LANES
        piece = source // LANES
        mean = (
            (piece == (target % LANES) // z.H)
            & (place // (2 * z.P) == target // LANES)
            & ((place % z.P) // 2 == target % z.H)
        )
        mean = jnp.where(mean, 0.125, 0.0).astype(jnp.bfloat16)

        def average(v, carry):
            columns = []
            for x in range(z.xc):
                for q in range(count):
                    blocks = []
                    for g in range(z.G):
                        i = q * z.G + g
                        blocks.append(
                            sums[v, i, pl.ds(2 * x, z.n, stride=z.xa), :] + sums[v, i, pl.ds(2 * x + 1, z.n, stride=z.xa), :]
                        )
                    columns.append(jnp.concatenate(blocks, axis=0))
            lhs = jnp.concatenate(parts(jnp.concatenate(columns, axis=1), 3), axis=0)
            got = jnp.dot(lhs, mean, preferred_element_type=jnp.float32)
            lines = z.G * z.n
            got = got[:lines] + got[lines : 2 * lines] + got[2 * lines :]
            for g in range(z.G):
                for h in range(half):
                    rows = pl.ds(v * z.H + half * g + h, z.n, stride=z.RA)
                    value = got[g * z.n : (g + 1) * z.n, h * LANES : (h + 1) * LANES]
                    avg[rows, :] = value
            return carry

        lax.fori_loop(0, 5, average, 0)


def provisional_kernel(z, columns, coarse, out, bare, outer, pad):
    rank = lax.axis_index("patch")
    row = lax.broadcasted_iota(jnp.int32, (z.R, LANES), 0)
    lane = lax.broadcasted_iota(jnp.int32, (z.R, LANES), 1)
    S = columns.shape[0]
    gy = columns[:, 0:1]
    turn = lax.broadcasted_iota(jnp.int32, (S, S), 0) == lax.broadcasted_iota(jnp.int32, (S, S), 1)
    gzr = jnp.sum(jnp.where(turn, columns[:, 1:2].astype(jnp.float32), 0.0), axis=0, keepdims=True).astype(jnp.int32)
    block = lambda a: (a + z.H) // z.H - 1
    place = lax.broadcasted_iota(jnp.int32, (z.R, S), 0) + rank * z.R
    across = lax.broadcasted_iota(jnp.int32, (S, LANES), 1)

    def uncovered(dz, dy):
        rows = (block(place + dz) == gzr + 1).astype(jnp.bfloat16)
        lanes = (block(across + dy) == gy + 1).astype(jnp.bfloat16)
        return 1.0 - jnp.dot(rows, lanes, preferred_element_type=jnp.float32)

    own, zu, zd, yu, yd = [uncovered(*shift) for shift in ((0, 0), (1, 0), (-1, 0), (0, 1), (0, -1))]
    zu = jnp.where(row < z.R - 1, zu, 0.0)
    zd = jnp.where(row > 0, zd, 0.0)
    bare[...] = own
    for v in range(5):
        outer[v, 0] = coarse[v, 0]
        outer[v, 1] = coarse[v, z.NX - 1]

    def layer(x, carry):
        U = [coarse[v, x] for v in range(5)]
        vel, pressure, sound = derived(U)
        last = jnp.minimum(x + 1, z.NX - 1)
        XU = [coarse[v, last] for v in range(5)]
        xvel, xp, xs = derived(XU)
        fx = twice_flux(U, (vel[0], pressure, sound), XU, (xvel[0], xp, xs), 0)
        inner = jnp.where(x < z.NX - 1, 1.0, 0.0)
        D = [vel[1], pressure, sound]
        move = lambda a: jnp.where(lane == LANES - 1, a, pltpu.roll(a, LANES - 1, 1))
        fy = twice_flux(U, D, [move(a) for a in U], [move(a) for a in D], 1)
        edge = twice_flux(U, D, U, D, 1)
        D = [vel[2], pressure, sound]
        move = lambda a: pltpu.roll(a, z.R - 1, 0)
        fz = twice_flux(U, D, [move(a) for a in U], [move(a) for a in D], 2)
        for v in range(5):
            face = fx[v] * inner
            below = jnp.where(x == 0, 0.0, pad[v])
            pad[v] = face
            ylow = jnp.where(lane == 0, edge[v], pltpu.roll(fy[v], 1, 1))
            zlow = pltpu.roll(fz[v], 1, 0)
            total = face - below + (fy[v] * yu - ylow * yd) + (fz[v] * zu - zlow * zd)
            out[v, x] = jnp.where(own > 0.0, U[v] - (0.5 * coarse_rate) * total, 0.0)
        return carry

    lax.fori_loop(0, z.NX, layer, 0)


def side_kernel(z, ids, columns, com, ghost, lat):
    S, f_of = z.S, z.P
    _, gy, gz, gyr, gzr = positions(z, ids, columns)
    lane = lax.broadcasted_iota(jnp.int32, (S, LANES), 1)
    kind = lane // f_of
    even = kind % 2 == 0
    steps = ((0, -1), (0, 1), (-1, 0), (1, 0))
    flags = [((gyr == gy + dy) & (gzr == gz + dz)).astype(jnp.float32) for dy, dz in steps]
    here = jnp.zeros((S, LANES), jnp.float32)
    for k in range(4):
        here = jnp.where(kind == k, jnp.sum(flags[k], axis=1, keepdims=True), here)
    picks = jnp.concatenate(flags, axis=1).astype(jnp.bfloat16)

    for i in range(z.n):
        for k in range(5 * z.xa):
            lat[k * S + i * z.own : k * S + (i + 1) * z.own, :] = com[i * z.RC + k * z.own : i * z.RC + (k + 1) * z.own, :]

    def onehot(index, extent):
        return (lax.broadcasted_iota(jnp.int32, (S, extent), 1) == index).astype(jnp.bfloat16)

    vx = 5 * z.xc
    low_lines = jnp.concatenate([com[pl.ds(z.OZ + 2 * k + 1, z.n, stride=z.RC), :] for k in range(vx)], axis=1)
    top_lines = jnp.concatenate([com[pl.ds(z.OZ + 2 * k, z.n, stride=z.RC), :] for k in range(vx)], axis=1)
    low_rows = select_dot(onehot(gz * z.m + z.m - 1, z.n), low_lines)
    top_rows = select_dot(onehot((gz + 2) * z.m, z.n), top_lines)
    y_index = z.H * (gy + 1) + (lane % f_of) // 2
    half = (lane % f_of) // 2
    y_rows = {}
    sides = ((2, 2 * gy + 1), (3, 2 * (gy + 2)))
    table = jnp.concatenate([com[i * z.RC + z.OY : i * z.RC + z.OY + z.lines, :] for i in range(z.n)], axis=0)
    rest = jnp.concatenate([com[i * z.RC + z.OT : i * z.RC + z.OT + 8, :] for i in range(z.n)], axis=0)
    quarter = z.lines // 4
    for h in range(z.m):
        for f, line in sides:
            source = (gz + 1) * z.m + h
            y_rows[0, h, f] = select_dot(onehot(source * z.lines + line, z.n * z.lines), table)
            if z.tail:
                y_rows[1, h, f] = select_dot(onehot(source * 8 + line % quarter, z.n * 8), rest)
    for v in range(5):
        swapped = []
        for a in range(z.xa):
            T = lat[(v * z.xa + a) * S : (v * z.xa + a + 1) * S, :]
            T = jnp.where(even, pltpu.roll(T, LANES - f_of, 1), pltpu.roll(T, f_of, 1))
            swapped.append(jnp.concatenate([jnp.where(kind == k, T, 0.0) for k in range(4)], axis=0))
        near = select_dot(picks, jnp.concatenate(swapped, axis=1))
        for x in range(z.xc):
            k = v * z.xc + x
            at = slice(k * LANES, (k + 1) * LANES)
            c = jnp.where(kind == 0, lanes_at(low_rows[:, at], y_index), lanes_at(top_rows[:, at], y_index))
            start = k * z.R
            for f, line in sides:
                base = start if start < LANES else start - LANES + (line // quarter) * z.tail
                for h in range(z.m):
                    got = lanes_at(y_rows[start // LANES, h, f], base + half % z.R)
                    c = jnp.where((kind == f) & (half // z.R == h), got, c)
            for a in (2 * x, 2 * x + 1):
                ghost[(v * z.xa + a) * S : (v * z.xa + a + 1) * S, :] = jnp.where(
                    here > 0.0, near[:, a * LANES : (a + 1) * LANES], c
                )

    is_z = kind < 2
    sign = jnp.where(even, 0.5 * fine_rate, -0.5 * fine_rate)
    for a in range(z.xa):
        at = [slice((v * z.xa + a) * S, (v * z.xa + a + 1) * S) for v in range(5)]
        own = [lat[s, :] for s in at]
        far = [ghost[s, :] for s in at]
        L = [jnp.where(even, far[v], own[v]) for v in range(5)]
        R = [jnp.where(even, own[v], far[v]) for v in range(5)]
        vl, pl_, cl = derived(L)
        vr, pr, cr = derived(R)
        sl = jnp.where(is_z, vl[2], vl[1])
        sr = jnp.where(is_z, vr[2], vr[1])
        F = twice_flux(L, (sl, pl_, cl), R, (sr, pr, cr), None)
        both = pl_ + pr
        F[2] = F[2] + jnp.where(is_z, 0.0, both)
        F[3] = F[3] + jnp.where(is_z, both, 0.0)
        for v in range(5):
            C = sign * F[v]
            ghost[at[v], :] = C


def end_kernel(z, ids, columns, com, ghost, below, above, outf, xc, xs):
    S = z.S
    slab = lax.axis_index("slab")
    number = positions(z, ids, columns)[0]
    for d in range(z.n):
        for k in range(5 * z.xa):
            outf[d * z.RF + k * z.own : d * z.RF + (k + 1) * z.own, :] = ghost[k * S + d * z.own : k * S + (d + 1) * z.own, :]
    for w, (source, pitch, offset) in enumerate(
        ((com, z.RC, z.OX), (com, z.RC, z.OX + 5 * z.own), (below, 5 * z.own, 0), (above, 5 * z.own, 0))
    ):
        for i in range(z.n):
            for v in range(5):
                k = (w * 5 + v) * S + i * z.own
                r = i * pitch + offset + v * z.own
                xs[k : k + z.own, :] = source[r : r + z.own, :]
    for side, (margin, edge) in enumerate(((below, slab == 0), (above, slab == z.slabs - 1))):
        match = (number == margin[z.OM + 5 * z.R : z.OM + 5 * z.R + 1, :S]).astype(jnp.bfloat16)
        own = [xs[(side * 5 + v) * S : (side * 5 + v + 1) * S, :] for v in range(5)]
        far = select_dot(
            match, jnp.concatenate([xs[((2 + side) * 5 + v) * S : ((2 + side) * 5 + v + 1) * S, :] for v in range(5)], axis=1)
        )
        far = [jnp.where(edge, own[v], far[:, v * LANES : (v + 1) * LANES]) for v in range(5)]
        F = state_flux(far, own, 0) if side == 0 else state_flux(own, far, 0)
        for v in range(5):
            C = (0.5 * fine_rate if side == 0 else -0.5 * fine_rate) * F[v]
            xc[(side * 5 + v) * S : (side * 5 + v + 1) * S, :] = C
            for d in range(z.n):
                k = d * z.RF + z.OFX + (side * 5 + v) * z.own
                outf[k : k + z.own, :] = C[d * z.own : (d + 1) * z.own]


def canvas_kernel(z, ids_s, columns_s, ids, columns, com, ghost, xc, avg, *rest):
    outs, (canvas, ends) = rest[: z.n], rest[z.n :]
    S, f_of = z.S, z.P
    vx = 5 * z.xc
    _, gy, gz, gyr, gzr = positions(z, ids, columns)
    lane = lax.broadcasted_iota(jnp.int32, (S, LANES), 1)
    steps = ((0, -1), (0, 1), (-1, 0), (1, 0))
    flags = [((gyr == gy + dy) & (gzr == gz + dz)).astype(jnp.float32) for dy, dz in steps]
    turned = [((gy == gyr + dy) & (gz == gzr + dz)).astype(jnp.float32) for dy, dz in steps]
    absent_row = [1.0 - jnp.sum(t, axis=0, keepdims=True) for t in turned]
    zrow = lax.broadcasted_iota(jnp.int32, (z.NZ, S), 0)
    base = z.H * (gzr + 1)
    zmat = jnp.concatenate(
        [
            (zrow == base).astype(jnp.float32) - absent_row[0] * (zrow == base - 1).astype(jnp.float32),
            (zrow == base + z.H - 1).astype(jnp.float32) - absent_row[1] * (zrow == base + z.H).astype(jnp.float32),
        ],
        axis=1,
    ).astype(jnp.bfloat16)
    ybase = z.H * (gy + 1)
    absent = [1.0 - jnp.sum(flags[k], axis=1, keepdims=True) for k in (2, 3)]
    ymat = jnp.concatenate(
        [
            (lane == ybase).astype(jnp.float32) - absent[0] * (lane == ybase - 1).astype(jnp.float32),
            (lane == ybase + z.H - 1).astype(jnp.float32) - absent[1] * (lane == ybase + z.H).astype(jnp.float32),
        ],
        axis=0,
    ).astype(jnp.bfloat16)
    in_y = lane // z.H == gy + 1
    in_z = lane // z.H == gz + 1
    zq, yq = [], []
    for v in range(5):
        for x in range(z.xc):
            r = (v * z.xa + 2 * x) * S
            Q = ghost[r : r + S, :] + ghost[r + S : r + 2 * S, :]
            Q = 0.125 * (Q + pltpu.roll(Q, LANES - 1, 1))
            got = [lanes_at(Q, f_of * f + 2 * (lane % z.H)) for f in range(4)]
            zq.append(jnp.concatenate([jnp.where(in_y, got[f], 0.0) for f in (0, 1)], axis=0))
            yq.append(jnp.concatenate([jnp.where(in_z, got[f], 0.0) for f in (2, 3)], axis=0))
    zsum = select_dot(zmat, jnp.concatenate(zq, axis=1), 2)
    ysum = None
    for piece in parts(jnp.concatenate([a.T for a in yq], axis=0), 2):
        term = jnp.dot(piece, ymat, preferred_element_type=jnp.float32)
        ysum = term if ysum is None else ysum + term
    for k in range(vx):
        canvas[k * z.NZ : (k + 1) * z.NZ, :] = zsum[:, k * LANES : (k + 1) * LANES] + ysum[k * z.NZ : (k + 1) * z.NZ, :]
    rank = lax.broadcasted_iota(jnp.int32, (z.n, LANES), 0)
    rank_slot = lax.broadcasted_iota(jnp.int32, (z.n, S), 0)
    inside_y = in_y.astype(jnp.bfloat16)
    cover = lambda block: jnp.dot((block == gzr + 1).astype(jnp.bfloat16), inside_y, preferred_element_type=jnp.float32)
    bare_first = 1.0 - cover((rank_slot * z.R) // z.H)
    bare_last = 1.0 - cover((rank_slot * z.R + z.R - 1) // z.H)
    low_mask = bare_first * jnp.where(rank == 0, 1.0, pltpu.roll(bare_last, 1, 0))
    top_mask = bare_last * jnp.where(rank == z.n - 1, 1.0, pltpu.roll(bare_first, z.n - 1, 0))
    for x in range(z.xc):
        lines = [[com[pl.ds(z.OZ + 2 * (v * z.xc + x) + s, z.n, stride=z.RC), :] for v in range(5)] for s in (0, 1)]
        under = [jnp.where(rank == 0, lines[0][v], pltpu.roll(lines[1][v], 1, 0)) for v in range(5)]
        over = [jnp.where(rank == z.n - 1, lines[1][v], pltpu.roll(lines[0][v], z.n - 1, 0)) for v in range(5)]
        low = state_flux(under, lines[0], 2)
        top = state_flux(lines[1], over, 2)
        for v in range(5):
            first = pl.ds((v * z.xc + x) * z.NZ, z.n, stride=z.R)
            last = pl.ds((v * z.xc + x) * z.NZ + z.R - 1, z.n, stride=z.R)
            canvas[first, :] = canvas[first, :] + (0.5 * coarse_rate) * low_mask * low[v]
            canvas[last, :] = canvas[last, :] - (0.5 * coarse_rate) * top_mask * top[v]

    spot = lax.broadcasted_iota(jnp.int32, (z.H, LANES), 1) // z.H

    def place(k, carry):
        i = k // z.own
        q = k % z.own
        sy = columns_s[ids_s[0, k], 0] + 1
        sz = columns_s[ids_s[0, k], 1] + 1
        inside = spot == sy
        for v in range(5):
            block = avg[pl.ds(pl.multiple_of(i * z.RA + v * z.H, 8), z.H), :]
            for x in range(z.xc):
                shift = lax.rem(z.H * (sy - (x * z.own + q)) + 2 * LANES, LANES)
                rows = pl.ds(pl.multiple_of((v * z.xc + x) * z.NZ + z.H * sz, z.H), z.H)
                canvas[rows, :] = canvas[rows, :] + jnp.where(inside, pltpu.roll(block, shift, 1), 0.0)
        return carry

    lax.fori_loop(0, S, place, 0, unroll=4)
    zb = (rank_slot // z.m == gzr + 1).astype(jnp.bfloat16)
    tops = []
    for side in range(2):
        for v in range(5):
            C = xc[(side * 5 + v) * S : (side * 5 + v + 1) * S, :]
            Q = C + pltpu.roll(C, LANES - 1, 1)
            Q = 0.125 * (Q + pltpu.roll(Q, LANES - z.P, 1))
            for h in range(z.zcl):
                tops.append(jnp.where(in_y, lanes_at(Q, 2 * z.P * h + 2 * (lane % z.H)), 0.0))
    tops = select_dot(zb, jnp.concatenate(tops, axis=1), 2)
    for e in range(10 * z.zcl):
        ends[e] = tops[:, e * LANES : (e + 1) * LANES]
    rank = lax.axis_index("patch")
    for k, out in enumerate(outs):
        d = lax.rem(rank + k, z.n)
        for e in range(vx):
            out[e * z.R : (e + 1) * z.R, :] = canvas[pl.ds(pl.multiple_of(e * z.NZ + d * z.R, 8), z.R), :]
        for e in range(10 * z.zcl):
            out[z.OXQ + e : z.OXQ + e + 1, :] = ends[e, pl.ds(d, 1), :]


def fine_kernel(z, updated, recv, out, scr):
    q = pl.program_id(0)
    lane = lax.broadcasted_iota(jnp.int32, (z.P, LANES), 1)
    y = lane % z.P
    edge = (y == 0) | (y == z.P - 1)
    pick = jnp.where(y == 0, 2 * z.P, 3 * z.P) + lane // z.P
    for v in range(5):
        for a in range(z.xa):
            scr[v % 2, pl.ds(a, z.n, stride=z.xa), :] = recv[pl.ds((v * z.xa + a) * z.own + q, z.n, stride=z.RF), :]
        face = scr[v % 2]
        for g in range(z.G):
            at = slice(g * LANES, (g + 1) * LANES)
            add = jnp.where(edge, lanes_at(face, jnp.where(edge, pick + z.zg * g, 0)), 0.0)
            if g == 0:
                add = add + jnp.where(lane < z.P, face, 0.0)
            if g == z.G - 1:
                add = add + jnp.where(lane >= LANES - z.P, pltpu.roll(face, 2 * z.P, 1), 0.0)
            out[v, 0, :, at] = updated[v, q, :, at] + add
        for side in range(2):
            x = side * (z.P - 1)
            for j in range(z.n):
                r = j * z.RF + z.OFX + (side * 5 + v) * z.own + q
                at = slice(j * z.PL, (j + 1) * z.PL)
                out[v, 0, x : x + 1, at] = out[v, 0, x : x + 1, at] + recv[pl.ds(r, 1), : z.PL]


def coarse_kernel(z, prov, bare, coarse, below, above, *rest):
    recv, out = rest[: z.n], rest[z.n]
    slab, rank = lax.axis_index("slab"), lax.axis_index("patch")
    offset = lax.rem(rank, z.m) * z.R
    for k in range(z.n):
        j = lax.rem(rank + z.n - k, z.n)
        for v in range(5):
            for x in range(z.xc):
                r = (v * z.xc + x) * z.R
                out[v, j * z.xc + x] = prov[v, j * z.xc + x] + recv[k][r : r + z.R, :]
    for side, margin, edge in ((0, below, slab == 0), (1, above, slab == z.slabs - 1)):
        x = side * (z.NX - 1)
        own = [coarse[v, side] for v in range(5)]
        far = [jnp.where(edge, own[v], margin[z.OM + v * z.R : z.OM + (v + 1) * z.R, :]) for v in range(5)]
        F = state_flux(far, own, 0) if side == 0 else state_flux(own, far, 0)
        scale = (0.5 if side == 0 else -0.5) * coarse_rate * bare[...]
        for v in range(5):
            out[v, x] = out[v, x] + scale * F[v]
    for k in range(z.n):
        j = lax.rem(rank + z.n - k, z.n)
        for h in range(z.zcl):
            row = j * z.zcl + h - offset
            inside = (row >= 0) & (row < z.R)
            row = jnp.clip(row, 0, z.R - 1)
            for v in range(5):
                for side in range(2):
                    x = side * (z.NX - 1)
                    r = z.OXQ + (side * 5 + v) * z.zcl + h
                    add = jnp.where(inside, recv[k][r : r + 1, :], 0.0)
                    out[v, x, pl.ds(row, 1), :] = out[v, x, pl.ds(row, 1), :] + add


def held(a, space=pltpu.VMEM):
    return pltpu.with_memory_space_constraint(a, space)


def call(kernel, z, outs, ins, scratch=(), keep=pltpu.VMEM):
    return pl.pallas_call(
        functools.partial(kernel, z),
        out_shape=[keep(s, jnp.float32) for s in outs],
        in_specs=[SMEM if space == "s" else VMEM for space, _ in ins],
        out_specs=[VMEM] * len(outs),
        scratch_shapes=[pltpu.VMEM(s, jnp.float32) for s in scratch],
        compiler_params=pltpu.CompilerParams(vmem_limit_bytes=VMEM_LIMIT),
    )(*[{"p": held(a), "h": held(a, pltpu.HBM)}.get(space, a) for space, a in ins])


def run_advance(z, fine):
    block = pl.BlockSpec((5, 1) + fine.shape[2:], lambda i: (0, i, 0, 0))
    average = (z.n * z.RA, LANES)
    return pl.pallas_call(
        functools.partial(advance_kernel, z),
        grid=(z.own,),
        out_shape=[pltpu.VMEM(fine.shape, jnp.float32), pltpu.HBM(average, jnp.float32)],
        in_specs=[block],
        out_specs=[VMEM, pl.BlockSpec(average, lambda i: (0, 0))],
        scratch_shapes=[
            pltpu.VMEM(s, jnp.float32)
            for s in ((10, z.G, z.P + 8, LANES), (5, z.P + 8, LANES), (5, z.P, LANES), (5, z.own * z.G, z.P, LANES))
        ],
        compiler_params=pltpu.CompilerParams(vmem_limit_bytes=VMEM_LIMIT),
        name="advance",
    )(fine)


def run_fine(z, updated, recv):
    block = pl.BlockSpec((5, 1) + updated.shape[2:], lambda i: (0, i, 0, 0))
    return pl.pallas_call(
        functools.partial(fine_kernel, z),
        grid=(z.own,),
        out_shape=jax.ShapeDtypeStruct(updated.shape, jnp.float32),
        in_specs=[VMEM, VMEM],
        out_specs=block,
        scratch_shapes=[pltpu.VMEM((2, z.P, LANES), jnp.float32)],
        compiler_params=pltpu.CompilerParams(vmem_limit_bytes=VMEM_LIMIT),
        name="fine_edges",
    )(held(updated), held(recv))


def local(n, slabs, coarse, fine, columns, patch_ids):
    return level_step(n, slabs, coarse, fine, columns, patch_ids)


def level_step(n, slabs, coarse, fine, columns, patch_ids):
    slots = patch_ids.shape[1]
    assert columns.shape[0] == slots
    z = Sizes(n, slabs, fine.shape, coarse.shape, slots)

    def exchange(a):
        return lax.all_to_all(a, "patch", 0, 0, tiled=True)

    def shifted(a, step):
        pairs = [(i, i + step) for i in range(slabs) if 0 <= i + step < slabs]
        return lax.ppermute(a, "slab", pairs)

    faces = (5 * z.xa * slots, LANES)
    (com,) = call(
        extract_kernel, z, [(n * z.RC, LANES)], [("h", fine), ("h", coarse)], [(2, z.P, LANES)], keep=pltpu.HBM
    )
    com = exchange(com)
    updated, avg = run_advance(z, fine)
    avg = exchange(avg)
    prov, bare, outer = call(
        provisional_kernel,
        z,
        [coarse.shape, (z.R, LANES), (5, 2, z.R, LANES)],
        [("v", columns), ("v", coarse)],
        [(5, z.R, LANES)],
    )
    up, dn = call(pack_kernel, z, [(z.RP, LANES)] * 2, [("p", com), ("p", outer), ("v", patch_ids)])
    below = shifted(up, 1)
    above = shifted(dn, -1)
    (ghost,) = call(side_kernel, z, [faces], [("v", patch_ids), ("v", columns), ("p", com)], [faces])
    outf, xc = call(
        end_kernel,
        z,
        [(n * z.RF, LANES), (10 * slots, LANES)],
        [("v", patch_ids), ("v", columns)] + [("p", a) for a in (com, ghost, below, above)],
        [(20 * slots, LANES)],
    )
    outf = exchange(outf)
    pieces = list(call(
        canvas_kernel,
        z,
        [(z.RK, LANES)] * n,
        [("s", patch_ids), ("s", columns), ("v", patch_ids), ("v", columns)]
        + [("p", a) for a in (com, ghost, xc, avg)],
        [(5 * z.xc * z.NZ, LANES), (10 * z.zcl, n, LANES)],
    ))
    for k in range(1, n):
        pieces[k] = lax.ppermute(pieces[k], "patch", [(i, (i + k) % n) for i in range(n)])
    fine_out = run_fine(z, updated, outf)
    (coarse_out,) = call(
        coarse_kernel,
        z,
        [coarse.shape],
        [("p", a) for a in (prov, bare, outer, below, above, *pieces)],
        keep=jax.ShapeDtypeStruct,
    )
    return coarse_out, fine_out


def solution(mesh):
    n, slabs = mesh.shape["patch"], mesh.shape["slab"]
    return jax.shard_map(
        functools.partial(local, n, slabs),
        mesh=mesh,
        in_specs=(
            P(None, "slab", "patch", None),
            P(None, ("slab", "patch"), None, None),
            P(),
            P("slab", None),
        ),
        out_specs=(P(None, "slab", "patch", None), P(None, ("slab", "patch"), None, None)),
        check_vma=False,
    )
```

```python
import functools

import jax
import jax.numpy as jnp
from jax import lax
from jax.experimental import pallas as pl
from jax.experimental.pallas import tpu as pltpu
from jax.sharding import PartitionSpec as P


LANES = 128
XROWS = 16
VMEM_LIMIT = 24 * 1024 * 1024
heat_ratio = 1.4
fine_rate = 0.1
coarse_rate = 0.05
VMEM = pl.BlockSpec(memory_space=pltpu.VMEM)
SMEM = pl.BlockSpec(memory_space=pltpu.SMEM)


def up8(count):
    return -(-count // 8) * 8


class Sizes:
    def __init__(self, n, slabs, fine_shape, coarse_shape, slots):
        self.n, self.slabs, self.S = n, slabs, slots
        self.own = fine_shape[1]
        self.P = fine_shape[2]
        self.cells = fine_shape[3]
        self.H = self.P // 2
        self.G = self.cells // LANES
        self.zg = LANES // self.P
        self.xa = self.P // n
        self.xc = self.H // n
        self.PL = self.cells // n
        self.zcl = self.P // n // 2
        self.NX, self.R, self.NY = coarse_shape[1:]
        self.m = self.H // self.R
        self.NZ = self.R * n
        self.lines = 2 * (self.NY // self.H)
        assert self.NX == self.H and self.NY == LANES and self.H % self.R == 0
        assert self.P % (2 * n) == 0 and 4 * self.P == LANES and slots == self.own * n
        self.lat = 5 * self.xa * self.own
        self.width = 5 * self.xc * self.R
        self.tail = max(self.width - LANES, 0)
        assert 4 * self.tail in (0, LANES)
        self.OY = up8(self.lat)
        self.OT = self.OY + self.lines
        self.OZ = self.OT + (self.lines // 4 if self.tail else 0)
        self.OX = self.OZ + 10 * self.xc
        self.RC = up8(self.OX + 10 * self.own)
        self.OM = up8(n * 5 * self.own)
        self.RA = 5 * self.H
        self.OFX = self.lat
        self.RF = up8(self.lat + 10 * self.own)
        self.OXQ = 5 * self.xc * self.R
        self.RK = up8(self.OXQ + 10 * self.zcl)
        self.RM = 5 * self.R + 8
        self.RP = self.OM + self.RM


def parts(x, count):
    out = []
    for _ in range(count):
        piece = x.astype(jnp.bfloat16)
        out.append(piece)
        x = x - piece.astype(jnp.float32)
    return out


def select_dot(pick, x, count=3, dims=(((1,), (0,)), ((), ()))):
    total = None
    for piece in parts(x, count):
        term = lax.dot_general(pick, piece, dims, preferred_element_type=jnp.float32)
        total = term if total is None else total + term
    return total


def lanes_at(x, index):
    return jnp.take_along_axis(x, index, axis=1, mode="promise_in_bounds")


def derived(U):
    inverse = 1.0 / U[0]
    velocity = [U[1] * inverse, U[2] * inverse, U[3] * inverse]
    kinetic = U[1] * velocity[0] + U[2] * velocity[1] + U[3] * velocity[2]
    pressure = (heat_ratio - 1.0) * (U[4] - 0.5 * kinetic)
    sound = jnp.sqrt(heat_ratio * pressure * inverse)
    return velocity, pressure, sound


def directed(U, speed, pressure, d):
    out = [U[0] * speed if d is None else U[1 + d]]
    out += [U[1 + e] * speed + (pressure if e == d else 0.0) if e == d else U[1 + e] * speed for e in range(3)]
    out.append((U[4] + pressure) * speed)
    return out


def twice_flux(L, dl, R, dr, d):
    fl = directed(L, dl[0], dl[1], d)
    fr = directed(R, dr[0], dr[1], d)
    signal = jnp.maximum(jnp.abs(dl[0]) + dl[2], jnp.abs(dr[0]) + dr[2])
    return [fl[v] + fr[v] - signal * (R[v] - L[v]) for v in range(5)]


def state_flux(L, R, d):
    vl, pl_, cl = derived(L)
    vr, pr, cr = derived(R)
    return twice_flux(L, (vl[d], pl_, cl), R, (vr[d], pr, cr), d)


def positions(z, ids, columns):
    down = lax.broadcasted_iota(jnp.int32, (z.S, z.S), 0)
    across = lax.broadcasted_iota(jnp.int32, (z.S, z.S), 1)
    number_row = ids[...].astype(jnp.float32)
    held = down.astype(jnp.float32) == number_row
    place = columns[...].astype(jnp.float32)
    rows = [jnp.sum(jnp.where(held, place[:, k : k + 1], 0.0), axis=0, keepdims=True) for k in range(2)]
    turn = lambda r: jnp.sum(jnp.where(down == across, r, 0.0), axis=1, keepdims=True)
    whole = lambda a: a.astype(jnp.int32)
    return turn(number_row), whole(turn(rows[0])), whole(turn(rows[1])), whole(rows[0]), whole(rows[1])


def extract_kernel(z, fine, coarse, com, scr):
    lane = lax.broadcasted_iota(jnp.int32, (z.P, LANES), 1)
    pick = z.P * ((lane % z.P) % z.zg) + jnp.where(lane >= 3 * z.P, z.P - 1, 0)
    group = jnp.where(lane >= 2 * z.P, (lane % z.P) // z.zg, -1)
    for q in range(z.own):
        for v in range(5):
            first = fine[v, q, :, :LANES]
            last = fine[v, q, :, (z.G - 1) * LANES :]
            face = jnp.where(lane < z.P, first, pltpu.roll(last, 2 * z.P, 1))
            for g in range(z.G):
                chunk = fine[v, q, :, g * LANES : (g + 1) * LANES]
                face = jnp.where(group == g, lanes_at(chunk, pick), face)
            scr[v % 2] = face
            for a in range(z.xa):
                com[pl.ds((v * z.xa + a) * z.own + q, z.n, stride=z.RC), :] = scr[v % 2, pl.ds(a, z.n, stride=z.xa), :]
            for side in range(2):
                row = fine[v, q, side * (z.P - 1) : side * (z.P - 1) + 1, :]
                place = z.OX + (side * 5 + v) * z.own + q
                for j in range(z.n):
                    com[j * z.RC + place : j * z.RC + place + 1, : z.PL] = row[:, j * z.PL : (j + 1) * z.PL]
    line = lax.broadcasted_iota(jnp.int32, (z.lines, LANES), 0)
    at = lax.broadcasted_iota(jnp.int32, (z.lines, LANES), 1)
    chosen = (at == z.H * (line // 2) + (z.H - 1) * (line % 2)).astype(jnp.bfloat16)
    quarter = z.lines // 4
    target = lax.broadcasted_iota(jnp.int32, (quarter, LANES), 1) // (LANES // 4)
    for j in range(z.n):
        block = coarse[:, j * z.xc : (j + 1) * z.xc].reshape(z.width, LANES)
        if z.tail:
            block = jnp.concatenate([block, jnp.zeros((2 * LANES - z.width, LANES), jnp.float32)], axis=0)
        lines = select_dot(chosen, block, 3, (((1,), (1,)), ((), ())))
        extent = min(LANES, z.width)
        com[j * z.RC + z.OY : j * z.RC + z.OY + z.lines, :extent] = lines[:, :extent]
        if z.tail:
            packed = jnp.zeros((quarter, LANES), jnp.float32)
            for b in range(4):
                moved = pltpu.roll(lines[:, LANES:], b * z.tail, 1)[b * quarter : (b + 1) * quarter]
                packed = jnp.where(target == b, moved, packed)
            com[j * z.RC + z.OT : j * z.RC + z.OT + quarter, :] = packed
        for v in range(5):
            for x in range(z.xc):
                row = j * z.RC + z.OZ + (v * z.xc + x) * 2
                com[row : row + 1, :] = coarse[v, j * z.xc + x, 0:1, :]
                com[row + 1 : row + 2, :] = coarse[v, j * z.xc + x, z.R - 1 : z.R, :]


def pack_kernel(z, com, outer, ids, up, dn):
    for side, margin in ((1, up), (0, dn)):
        for i in range(z.n):
            k = i * z.RC + z.OX + side * 5 * z.own
            margin[i * 5 * z.own : (i + 1) * 5 * z.own, :] = com[k : k + 5 * z.own, :]
        for v in range(5):
            margin[z.OM + v * z.R : z.OM + (v + 1) * z.R, :] = outer[v, side]
        margin[z.OM + 5 * z.R : z.OM + 5 * z.R + 8, :] = jnp.zeros((8, LANES), jnp.float32)
        margin[z.OM + 5 * z.R : z.OM + 5 * z.R + 1, : z.S] = ids[...].astype(jnp.float32)


def advance_kernel(z, fine, updated, avg, work, xflux, zflux, sums):
    count = z.own
    patch = pl.program_id(0)
    X = min(XROWS, z.P)
    lane = lax.broadcasted_iota(jnp.int32, (X, LANES), 1)
    row = lax.broadcasted_iota(jnp.int32, (X, LANES), 0)
    inner_y = lane % z.P < z.P - 1
    first_z = lane < z.P

    def first_pass(i, carry):
        at = pl.ds(pl.multiple_of(i * LANES, LANES), LANES)
        U = [fine[v, 0, :, at] for v in range(5)]
        velocity, pressure, sound = derived(U)
        for k, value in enumerate(U + velocity + [pressure, sound]):
            work[k, i, : z.P, :] = value
        return carry

    lax.fori_loop(0, z.G, first_pass, 0)
    xflux[:, :8, :] = jnp.zeros((5, 8, LANES), jnp.float32)

    def second_pass(i, carry):
        at = pl.ds(pl.multiple_of(i * LANES, LANES), LANES)
        nxt = jnp.minimum(i + 1, z.G - 1)
        inner_z = jnp.logical_or(lane < LANES - z.P, i < z.G - 1)
        for r in range(0, z.P, X):
            rows = slice(r, r + X)
            U = [work[k, i, rows, :] for k in range(5)]
            D = [work[k, i, rows, :] for k in range(5, 10)]
            XU = [work[k, i, r + 1 : r + 1 + X, :] for k in range(5)]
            XD = [work[k, i, r + 1 : r + 1 + X, :] for k in (5, 8, 9)]
            F = twice_flux(U, (D[0], D[3], D[4]), XU, XD, 0)
            change = []
            for v in range(5):
                face = jnp.where(row < z.P - 1 - r, F[v], 0.0) if r + X == z.P else F[v]
                xflux[v, 8 + r : 8 + r + X, :] = face
                change.append(face - xflux[v, 7 + r : 7 + r + X, :])
            ahead = lambda a: pltpu.roll(a, LANES - 1, 1)
            F = twice_flux(U, (D[1], D[3], D[4]), [ahead(a) for a in U], [ahead(D[k]) for k in (1, 3, 4)], 1)
            for v in range(5):
                face = jnp.where(inner_y, F[v], 0.0)
                change[v] = change[v] + (face - pltpu.roll(face, 1, 1))
            beyond = lambda k, a: pltpu.roll(jnp.where(first_z, work[k, nxt, rows, :], a), LANES - z.P, 1)
            F = twice_flux(
                U,
                (D[2], D[3], D[4]),
                [beyond(k, U[k]) for k in range(5)],
                [beyond(5 + k, D[k]) for k in (2, 3, 4)],
                2,
            )
            for v in range(5):
                face = jnp.where(inner_z, F[v], 0.0)
                rolled = pltpu.roll(face, z.P, 1)
                before = jnp.where(i == 0, 0.0, zflux[v, rows, :])
                zflux[v, rows, :] = rolled
                new = U[v] - (0.5 * fine_rate) * (change[v] + (face - jnp.where(first_z, before, rolled)))
                updated[v, patch, rows, at] = new
                sums[v, patch * z.G + i, rows, :] = new
        return carry

    lax.fori_loop(0, z.G, second_pass, 0)

    @pl.when(patch == count - 1)
    def _():
        half = z.zg // 2
        depth = z.xc * count * LANES
        source = lax.broadcasted_iota(jnp.int32, (depth, half * LANES), 0)
        target = lax.broadcasted_iota(jnp.int32, (depth, half * LANES), 1)
        place = source % LANES
        piece = source // LANES
        mean = (
            (piece == (target % LANES) // z.H)
            & (place // (2 * z.P) == target // LANES)
            & ((place % z.P) // 2 == target % z.H)
        )
        mean = jnp.where(mean, 0.125, 0.0).astype(jnp.bfloat16)

        def average(v, carry):
            columns = []
            for x in range(z.xc):
                for q in range(count):
                    blocks = []
                    for g in range(z.G):
                        i = q * z.G + g
                        blocks.append(
                            sums[v, i, pl.ds(2 * x, z.n, stride=z.xa), :] + sums[v, i, pl.ds(2 * x + 1, z.n, stride=z.xa), :]
                        )
                    columns.append(jnp.concatenate(blocks, axis=0))
            lhs = jnp.concatenate(parts(jnp.concatenate(columns, axis=1), 3), axis=0)
            got = jnp.dot(lhs, mean, preferred_element_type=jnp.float32)
            lines = z.G * z.n
            got = got[:lines] + got[lines : 2 * lines] + got[2 * lines :]
            for g in range(z.G):
                for h in range(half):
                    rows = pl.ds(v * z.H + half * g + h, z.n, stride=z.RA)
                    value = got[g * z.n : (g + 1) * z.n, h * LANES : (h + 1) * LANES]
                    avg[rows, :] = value
            return carry

        lax.fori_loop(0, 5, average, 0)


def provisional_kernel(z, columns, coarse, out, bare, outer, pad):
    rank = lax.axis_index("patch")
    row = lax.broadcasted_iota(jnp.int32, (z.R, LANES), 0)
    lane = lax.broadcasted_iota(jnp.int32, (z.R, LANES), 1)
    S = columns.shape[0]
    gy = columns[:, 0:1]
    turn = lax.broadcasted_iota(jnp.int32, (S, S), 0) == lax.broadcasted_iota(jnp.int32, (S, S), 1)
    gzr = jnp.sum(jnp.where(turn, columns[:, 1:2].astype(jnp.float32), 0.0), axis=0, keepdims=True).astype(jnp.int32)
    block = lambda a: (a + z.H) // z.H - 1
    place = lax.broadcasted_iota(jnp.int32, (z.R, S), 0) + rank * z.R
    across = lax.broadcasted_iota(jnp.int32, (S, LANES), 1)

    def uncovered(dz, dy):
        rows = (block(place + dz) == gzr + 1).astype(jnp.bfloat16)
        lanes = (block(across + dy) == gy + 1).astype(jnp.bfloat16)
        return 1.0 - jnp.dot(rows, lanes, preferred_element_type=jnp.float32)

    own, zu, zd, yu, yd = [uncovered(*shift) for shift in ((0, 0), (1, 0), (-1, 0), (0, 1), (0, -1))]
    zu = jnp.where(row < z.R - 1, zu, 0.0)
    zd = jnp.where(row > 0, zd, 0.0)
    bare[...] = own
    for v in range(5):
        outer[v, 0] = coarse[v, 0]
        outer[v, 1] = coarse[v, z.NX - 1]

    def layer(x, carry):
        U = [coarse[v, x] for v in range(5)]
        vel, pressure, sound = derived(U)
        last = jnp.minimum(x + 1, z.NX - 1)
        XU = [coarse[v, last] for v in range(5)]
        xvel, xp, xs = derived(XU)
        fx = twice_flux(U, (vel[0], pressure, sound), XU, (xvel[0], xp, xs), 0)
        inner = jnp.where(x < z.NX - 1, 1.0, 0.0)
        D = [vel[1], pressure, sound]
        move = lambda a: jnp.where(lane == LANES - 1, a, pltpu.roll(a, LANES - 1, 1))
        fy = twice_flux(U, D, [move(a) for a in U], [move(a) for a in D], 1)
        edge = twice_flux(U, D, U, D, 1)
        D = [vel[2], pressure, sound]
        move = lambda a: pltpu.roll(a, z.R - 1, 0)
        fz = twice_flux(U, D, [move(a) for a in U], [move(a) for a in D], 2)
        for v in range(5):
            face = fx[v] * inner
            below = jnp.where(x == 0, 0.0, pad[v])
            pad[v] = face
            ylow = jnp.where(lane == 0, edge[v], pltpu.roll(fy[v], 1, 1))
            zlow = pltpu.roll(fz[v], 1, 0)
            total = face - below + (fy[v] * yu - ylow * yd) + (fz[v] * zu - zlow * zd)
            out[v, x] = jnp.where(own > 0.0, U[v] - (0.5 * coarse_rate) * total, 0.0)
        return carry

    lax.fori_loop(0, z.NX, layer, 0)


def side_kernel(z, ids, columns, com, ghost, lat):
    S, f_of = z.S, z.P
    _, gy, gz, gyr, gzr = positions(z, ids, columns)
    lane = lax.broadcasted_iota(jnp.int32, (S, LANES), 1)
    kind = lane // f_of
    even = kind % 2 == 0
    steps = ((0, -1), (0, 1), (-1, 0), (1, 0))
    flags = [((gyr == gy + dy) & (gzr == gz + dz)).astype(jnp.float32) for dy, dz in steps]
    here = jnp.zeros((S, LANES), jnp.float32)
    for k in range(4):
        here = jnp.where(kind == k, jnp.sum(flags[k], axis=1, keepdims=True), here)
    picks = jnp.concatenate(flags, axis=1).astype(jnp.bfloat16)

    for i in range(z.n):
        for k in range(5 * z.xa):
            lat[k * S + i * z.own : k * S + (i + 1) * z.own, :] = com[i * z.RC + k * z.own : i * z.RC + (k + 1) * z.own, :]

    def onehot(index, extent):
        return (lax.broadcasted_iota(jnp.int32, (S, extent), 1) == index).astype(jnp.bfloat16)

    vx = 5 * z.xc
    low_lines = jnp.concatenate([com[pl.ds(z.OZ + 2 * k + 1, z.n, stride=z.RC), :] for k in range(vx)], axis=1)
    top_lines = jnp.concatenate([com[pl.ds(z.OZ + 2 * k, z.n, stride=z.RC), :] for k in range(vx)], axis=1)
    low_rows = select_dot(onehot(gz * z.m + z.m - 1, z.n), low_lines)
    top_rows = select_dot(onehot((gz + 2) * z.m, z.n), top_lines)
    y_index = z.H * (gy + 1) + (lane % f_of) // 2
    half = (lane % f_of) // 2
    y_rows = {}
    sides = ((2, 2 * gy + 1), (3, 2 * (gy + 2)))
    table = jnp.concatenate([com[i * z.RC + z.OY : i * z.RC + z.OY + z.lines, :] for i in range(z.n)], axis=0)
    rest = jnp.concatenate([com[i * z.RC + z.OT : i * z.RC + z.OT + 8, :] for i in range(z.n)], axis=0)
    quarter = z.lines // 4
    for h in range(z.m):
        for f, line in sides:
            source = (gz + 1) * z.m + h
            y_rows[0, h, f] = select_dot(onehot(source * z.lines + line, z.n * z.lines), table)
            if z.tail:
                y_rows[1, h, f] = select_dot(onehot(source * 8 + line % quarter, z.n * 8), rest)
    for v in range(5):
        swapped = []
        for a in range(z.xa):
            T = lat[(v * z.xa + a) * S : (v * z.xa + a + 1) * S, :]
            T = jnp.where(even, pltpu.roll(T, LANES - f_of, 1), pltpu.roll(T, f_of, 1))
            swapped.append(jnp.concatenate([jnp.where(kind == k, T, 0.0) for k in range(4)], axis=0))
        near = select_dot(picks, jnp.concatenate(swapped, axis=1))
        for x in range(z.xc):
            k = v * z.xc + x
            at = slice(k * LANES, (k + 1) * LANES)
            c = jnp.where(kind == 0, lanes_at(low_rows[:, at], y_index), lanes_at(top_rows[:, at], y_index))
            start = k * z.R
            for f, line in sides:
                base = start if start < LANES else start - LANES + (line // quarter) * z.tail
                for h in range(z.m):
                    got = lanes_at(y_rows[start // LANES, h, f], base + half % z.R)
                    c = jnp.where((kind == f) & (half // z.R == h), got, c)
            for a in (2 * x, 2 * x + 1):
                ghost[(v * z.xa + a) * S : (v * z.xa + a + 1) * S, :] = jnp.where(
                    here > 0.0, near[:, a * LANES : (a + 1) * LANES], c
                )

    is_z = kind < 2
    sign = jnp.where(even, 0.5 * fine_rate, -0.5 * fine_rate)
    for a in range(z.xa):
        at = [slice((v * z.xa + a) * S, (v * z.xa + a + 1) * S) for v in range(5)]
        own = [lat[s, :] for s in at]
        far = [ghost[s, :] for s in at]
        L = [jnp.where(even, far[v], own[v]) for v in range(5)]
        R = [jnp.where(even, own[v], far[v]) for v in range(5)]
        vl, pl_, cl = derived(L)
        vr, pr, cr = derived(R)
        sl = jnp.where(is_z, vl[2], vl[1])
        sr = jnp.where(is_z, vr[2], vr[1])
        F = twice_flux(L, (sl, pl_, cl), R, (sr, pr, cr), None)
        both = pl_ + pr
        F[2] = F[2] + jnp.where(is_z, 0.0, both)
        F[3] = F[3] + jnp.where(is_z, both, 0.0)
        for v in range(5):
            C = sign * F[v]
            ghost[at[v], :] = C


def end_kernel(z, ids, columns, com, ghost, below, above, outf, xc, xs):
    S = z.S
    slab = lax.axis_index("slab")
    number = positions(z, ids, columns)[0]
    for d in range(z.n):
        for k in range(5 * z.xa):
            outf[d * z.RF + k * z.own : d * z.RF + (k + 1) * z.own, :] = ghost[k * S + d * z.own : k * S + (d + 1) * z.own, :]
    for w, (source, pitch, offset) in enumerate(
        ((com, z.RC, z.OX), (com, z.RC, z.OX + 5 * z.own), (below, 5 * z.own, 0), (above, 5 * z.own, 0))
    ):
        for i in range(z.n):
            for v in range(5):
                k = (w * 5 + v) * S + i * z.own
                r = i * pitch + offset + v * z.own
                xs[k : k + z.own, :] = source[r : r + z.own, :]
    for side, (margin, edge) in enumerate(((below, slab == 0), (above, slab == z.slabs - 1))):
        match = (number == margin[z.OM + 5 * z.R : z.OM + 5 * z.R + 1, :S]).astype(jnp.bfloat16)
        own = [xs[(side * 5 + v) * S : (side * 5 + v + 1) * S, :] for v in range(5)]
        far = select_dot(
            match, jnp.concatenate([xs[((2 + side) * 5 + v) * S : ((2 + side) * 5 + v + 1) * S, :] for v in range(5)], axis=1)
        )
        far = [jnp.where(edge, own[v], far[:, v * LANES : (v + 1) * LANES]) for v in range(5)]
        F = state_flux(far, own, 0) if side == 0 else state_flux(own, far, 0)
        for v in range(5):
            C = (0.5 * fine_rate if side == 0 else -0.5 * fine_rate) * F[v]
            xc[(side * 5 + v) * S : (side * 5 + v + 1) * S, :] = C
            for d in range(z.n):
                k = d * z.RF + z.OFX + (side * 5 + v) * z.own
                outf[k : k + z.own, :] = C[d * z.own : (d + 1) * z.own]


def correct_kernel(z, ids, columns, ghost, canvas):
    S, f_of = z.S, z.P
    vx = 5 * z.xc
    _, gy, gz, gyr, gzr = positions(z, ids, columns)
    lane = lax.broadcasted_iota(jnp.int32, (S, LANES), 1)
    steps = ((0, -1), (0, 1), (-1, 0), (1, 0))
    flags = [((gyr == gy + dy) & (gzr == gz + dz)).astype(jnp.float32) for dy, dz in steps]
    turned = [((gy == gyr + dy) & (gz == gzr + dz)).astype(jnp.float32) for dy, dz in steps]
    absent_row = [1.0 - jnp.sum(t, axis=0, keepdims=True) for t in turned]
    zrow = lax.broadcasted_iota(jnp.int32, (z.NZ, S), 0)
    base = z.H * (gzr + 1)
    zmat = jnp.concatenate(
        [
            (zrow == base).astype(jnp.float32) - absent_row[0] * (zrow == base - 1).astype(jnp.float32),
            (zrow == base + z.H - 1).astype(jnp.float32) - absent_row[1] * (zrow == base + z.H).astype(jnp.float32),
        ],
        axis=1,
    ).astype(jnp.bfloat16)
    ybase = z.H * (gy + 1)
    absent = [1.0 - jnp.sum(flags[k], axis=1, keepdims=True) for k in (2, 3)]
    ymat = jnp.concatenate(
        [
            (lane == ybase).astype(jnp.float32) - absent[0] * (lane == ybase - 1).astype(jnp.float32),
            (lane == ybase + z.H - 1).astype(jnp.float32) - absent[1] * (lane == ybase + z.H).astype(jnp.float32),
        ],
        axis=0,
    ).astype(jnp.bfloat16)
    in_y = lane // z.H == gy + 1
    in_z = lane // z.H == gz + 1
    zq, yq = [], []
    for v in range(5):
        for x in range(z.xc):
            r = (v * z.xa + 2 * x) * S
            Q = ghost[r : r + S, :] + ghost[r + S : r + 2 * S, :]
            Q = 0.125 * (Q + pltpu.roll(Q, LANES - 1, 1))
            got = [lanes_at(Q, f_of * f + 2 * (lane % z.H)) for f in range(4)]
            zq.append(jnp.concatenate([jnp.where(in_y, got[f], 0.0) for f in (0, 1)], axis=0))
            yq.append(jnp.concatenate([jnp.where(in_z, got[f], 0.0) for f in (2, 3)], axis=0))
    zsum = select_dot(zmat, jnp.concatenate(zq, axis=1), 2)
    ysum = None
    for piece in parts(jnp.concatenate([a.T for a in yq], axis=0), 2):
        term = jnp.dot(piece, ymat, preferred_element_type=jnp.float32)
        ysum = term if ysum is None else ysum + term
    for k in range(vx):
        canvas[k * z.NZ : (k + 1) * z.NZ, :] = zsum[:, k * LANES : (k + 1) * LANES] + ysum[k * z.NZ : (k + 1) * z.NZ, :]


def canvas_kernel(z, ids_s, columns_s, ids, columns, com, start, xc, avg, *rest):
    outs, (canvas, ends) = rest[: z.n], rest[z.n :]
    S = z.S
    vx = 5 * z.xc
    _, gy, _, _, gzr = positions(z, ids, columns)
    lane = lax.broadcasted_iota(jnp.int32, (S, LANES), 1)
    in_y = lane // z.H == gy + 1
    canvas[...] = start[...]
    rank = lax.broadcasted_iota(jnp.int32, (z.n, LANES), 0)
    rank_slot = lax.broadcasted_iota(jnp.int32, (z.n, S), 0)
    inside_y = in_y.astype(jnp.bfloat16)
    cover = lambda block: jnp.dot((block == gzr + 1).astype(jnp.bfloat16), inside_y, preferred_element_type=jnp.float32)
    bare_first = 1.0 - cover((rank_slot * z.R) // z.H)
    bare_last = 1.0 - cover((rank_slot * z.R + z.R - 1) // z.H)
    low_mask = bare_first * jnp.where(rank == 0, 1.0, pltpu.roll(bare_last, 1, 0))
    top_mask = bare_last * jnp.where(rank == z.n - 1, 1.0, pltpu.roll(bare_first, z.n - 1, 0))
    for x in range(z.xc):
        lines = [[com[pl.ds(z.OZ + 2 * (v * z.xc + x) + s, z.n, stride=z.RC), :] for v in range(5)] for s in (0, 1)]
        under = [jnp.where(rank == 0, lines[0][v], pltpu.roll(lines[1][v], 1, 0)) for v in range(5)]
        over = [jnp.where(rank == z.n - 1, lines[1][v], pltpu.roll(lines[0][v], z.n - 1, 0)) for v in range(5)]
        low = state_flux(under, lines[0], 2)
        top = state_flux(lines[1], over, 2)
        for v in range(5):
            first = pl.ds((v * z.xc + x) * z.NZ, z.n, stride=z.R)
            last = pl.ds((v * z.xc + x) * z.NZ + z.R - 1, z.n, stride=z.R)
            canvas[first, :] = canvas[first, :] + (0.5 * coarse_rate) * low_mask * low[v]
            canvas[last, :] = canvas[last, :] - (0.5 * coarse_rate) * top_mask * top[v]

    spot = lax.broadcasted_iota(jnp.int32, (z.H, LANES), 1) // z.H

    def place(k, carry):
        i = k // z.own
        q = k % z.own
        sy = columns_s[ids_s[0, k], 0] + 1
        sz = columns_s[ids_s[0, k], 1] + 1
        inside = spot == sy
        for v in range(5):
            block = avg[pl.ds(pl.multiple_of(i * z.RA + v * z.H, 8), z.H), :]
            for x in range(z.xc):
                shift = lax.rem(z.H * (sy - (x * z.own + q)) + 2 * LANES, LANES)
                rows = pl.ds(pl.multiple_of((v * z.xc + x) * z.NZ + z.H * sz, z.H), z.H)
                canvas[rows, :] = canvas[rows, :] + jnp.where(inside, pltpu.roll(block, shift, 1), 0.0)
        return carry

    lax.fori_loop(0, S, place, 0, unroll=4)
    zb = (rank_slot // z.m == gzr + 1).astype(jnp.bfloat16)
    tops = []
    for side in range(2):
        for v in range(5):
            C = xc[(side * 5 + v) * S : (side * 5 + v + 1) * S, :]
            Q = C + pltpu.roll(C, LANES - 1, 1)
            Q = 0.125 * (Q + pltpu.roll(Q, LANES - z.P, 1))
            for h in range(z.zcl):
                tops.append(jnp.where(in_y, lanes_at(Q, 2 * z.P * h + 2 * (lane % z.H)), 0.0))
    tops = select_dot(zb, jnp.concatenate(tops, axis=1), 2)
    for e in range(10 * z.zcl):
        ends[e] = tops[:, e * LANES : (e + 1) * LANES]
    rank = lax.axis_index("patch")
    for k, out in enumerate(outs):
        d = lax.rem(rank + k, z.n)
        for e in range(vx):
            out[e * z.R : (e + 1) * z.R, :] = canvas[pl.ds(pl.multiple_of(e * z.NZ + d * z.R, 8), z.R), :]
        for e in range(10 * z.zcl):
            out[z.OXQ + e : z.OXQ + e + 1, :] = ends[e, pl.ds(d, 1), :]


def fine_kernel(z, updated, recv, out, scr):
    q = pl.program_id(0)
    lane = lax.broadcasted_iota(jnp.int32, (z.P, LANES), 1)
    y = lane % z.P
    edge = (y == 0) | (y == z.P - 1)
    pick = jnp.where(y == 0, 2 * z.P, 3 * z.P) + lane // z.P
    for v in range(5):
        for a in range(z.xa):
            scr[v % 2, pl.ds(a, z.n, stride=z.xa), :] = recv[pl.ds((v * z.xa + a) * z.own + q, z.n, stride=z.RF), :]
        face = scr[v % 2]
        for g in range(z.G):
            at = slice(g * LANES, (g + 1) * LANES)
            add = jnp.where(edge, lanes_at(face, jnp.where(edge, pick + z.zg * g, 0)), 0.0)
            if g == 0:
                add = add + jnp.where(lane < z.P, face, 0.0)
            if g == z.G - 1:
                add = add + jnp.where(lane >= LANES - z.P, pltpu.roll(face, 2 * z.P, 1), 0.0)
            out[v, 0, :, at] = updated[v, q, :, at] + add
        for side in range(2):
            x = side * (z.P - 1)
            for j in range(z.n):
                r = j * z.RF + z.OFX + (side * 5 + v) * z.own + q
                at = slice(j * z.PL, (j + 1) * z.PL)
                out[v, 0, x : x + 1, at] = out[v, 0, x : x + 1, at] + recv[pl.ds(r, 1), : z.PL]


def coarse_kernel(z, prov, bare, coarse, below, above, *rest):
    recv, out = rest[: z.n], rest[z.n]
    slab, rank = lax.axis_index("slab"), lax.axis_index("patch")
    offset = lax.rem(rank, z.m) * z.R
    for k in range(z.n):
        j = lax.rem(rank + z.n - k, z.n)
        for v in range(5):
            for x in range(z.xc):
                r = (v * z.xc + x) * z.R
                out[v, j * z.xc + x] = prov[v, j * z.xc + x] + recv[k][r : r + z.R, :]
    for side, margin, edge in ((0, below, slab == 0), (1, above, slab == z.slabs - 1)):
        x = side * (z.NX - 1)
        own = [coarse[v, side] for v in range(5)]
        far = [jnp.where(edge, own[v], margin[z.OM + v * z.R : z.OM + (v + 1) * z.R, :]) for v in range(5)]
        F = state_flux(far, own, 0) if side == 0 else state_flux(own, far, 0)
        scale = (0.5 if side == 0 else -0.5) * coarse_rate * bare[...]
        for v in range(5):
            out[v, x] = out[v, x] + scale * F[v]
    for k in range(z.n):
        j = lax.rem(rank + z.n - k, z.n)
        for h in range(z.zcl):
            row = j * z.zcl + h - offset
            inside = (row >= 0) & (row < z.R)
            row = jnp.clip(row, 0, z.R - 1)
            for v in range(5):
                for side in range(2):
                    x = side * (z.NX - 1)
                    r = z.OXQ + (side * 5 + v) * z.zcl + h
                    add = jnp.where(inside, recv[k][r : r + 1, :], 0.0)
                    out[v, x, pl.ds(row, 1), :] = out[v, x, pl.ds(row, 1), :] + add


def held(a, space=pltpu.VMEM):
    return pltpu.with_memory_space_constraint(a, space)


def call(kernel, z, outs, ins, scratch=(), keep=pltpu.VMEM):
    return pl.pallas_call(
        functools.partial(kernel, z),
        out_shape=[keep(s, jnp.float32) for s in outs],
        in_specs=[SMEM if space == "s" else VMEM for space, _ in ins],
        out_specs=[VMEM] * len(outs),
        scratch_shapes=[pltpu.VMEM(s, jnp.float32) for s in scratch],
        compiler_params=pltpu.CompilerParams(vmem_limit_bytes=VMEM_LIMIT),
    )(*[{"p": held(a), "h": held(a, pltpu.HBM)}.get(space, a) for space, a in ins])


def run_advance(z, fine):
    block = pl.BlockSpec((5, 1) + fine.shape[2:], lambda i: (0, i, 0, 0))
    average = (z.n * z.RA, LANES)
    return pl.pallas_call(
        functools.partial(advance_kernel, z),
        grid=(z.own,),
        out_shape=[pltpu.VMEM(fine.shape, jnp.float32), pltpu.HBM(average, jnp.float32)],
        in_specs=[block],
        out_specs=[VMEM, pl.BlockSpec(average, lambda i: (0, 0))],
        scratch_shapes=[
            pltpu.VMEM(s, jnp.float32)
            for s in ((10, z.G, z.P + 8, LANES), (5, z.P + 8, LANES), (5, z.P, LANES), (5, z.own * z.G, z.P, LANES))
        ],
        compiler_params=pltpu.CompilerParams(vmem_limit_bytes=VMEM_LIMIT),
        name="advance",
    )(fine)


def run_fine(z, updated, recv):
    block = pl.BlockSpec((5, 1) + updated.shape[2:], lambda i: (0, i, 0, 0))
    return pl.pallas_call(
        functools.partial(fine_kernel, z),
        grid=(z.own,),
        out_shape=jax.ShapeDtypeStruct(updated.shape, jnp.float32),
        in_specs=[VMEM, VMEM],
        out_specs=block,
        scratch_shapes=[pltpu.VMEM((2, z.P, LANES), jnp.float32)],
        compiler_params=pltpu.CompilerParams(vmem_limit_bytes=VMEM_LIMIT),
        name="fine_edges",
    )(held(updated), held(recv))


def local(n, slabs, coarse, fine, columns, patch_ids):
    return level_step(n, slabs, coarse, fine, columns, patch_ids)


def level_step(n, slabs, coarse, fine, columns, patch_ids):
    slots = patch_ids.shape[1]
    assert columns.shape[0] == slots
    z = Sizes(n, slabs, fine.shape, coarse.shape, slots)

    def exchange(a):
        return lax.all_to_all(a, "patch", 0, 0, tiled=True)

    def shifted(a, step):
        pairs = [(i, i + step) for i in range(slabs) if 0 <= i + step < slabs]
        return lax.ppermute(a, "slab", pairs)

    faces = (5 * z.xa * slots, LANES)
    (com,) = call(
        extract_kernel, z, [(n * z.RC, LANES)], [("h", fine), ("h", coarse)], [(2, z.P, LANES)], keep=pltpu.HBM
    )
    com = exchange(com)
    updated, avg = run_advance(z, fine)
    avg = exchange(avg)
    prov, bare, outer = call(
        provisional_kernel,
        z,
        [coarse.shape, (z.R, LANES), (5, 2, z.R, LANES)],
        [("v", columns), ("v", coarse)],
        [(5, z.R, LANES)],
    )
    up, dn = call(pack_kernel, z, [(z.RP, LANES)] * 2, [("p", com), ("p", outer), ("v", patch_ids)])
    below = shifted(up, 1)
    above = shifted(dn, -1)
    (ghost,) = call(side_kernel, z, [faces], [("v", patch_ids), ("v", columns), ("p", com)], [faces])
    (start,) = call(correct_kernel, z, [(5 * z.xc * z.NZ, LANES)], [("v", patch_ids), ("v", columns), ("p", ghost)])
    outf, xc = call(
        end_kernel,
        z,
        [(n * z.RF, LANES), (10 * slots, LANES)],
        [("v", patch_ids), ("v", columns)] + [("p", a) for a in (com, ghost, below, above)],
        [(20 * slots, LANES)],
    )
    outf = exchange(outf)
    pieces = list(call(
        canvas_kernel,
        z,
        [(z.RK, LANES)] * n,
        [("s", patch_ids), ("s", columns), ("v", patch_ids), ("v", columns)]
        + [("p", a) for a in (com, start, xc, avg)],
        [(5 * z.xc * z.NZ, LANES), (10 * z.zcl, n, LANES)],
    ))
    for k in range(1, n):
        pieces[k] = lax.ppermute(pieces[k], "patch", [(i, (i + k) % n) for i in range(n)])
    fine_out = run_fine(z, updated, outf)
    (coarse_out,) = call(
        coarse_kernel,
        z,
        [coarse.shape],
        [("p", a) for a in (prov, bare, outer, below, above, *pieces)],
        keep=jax.ShapeDtypeStruct,
    )
    return coarse_out, fine_out


def solution(mesh):
    n, slabs = mesh.shape["patch"], mesh.shape["slab"]
    return jax.shard_map(
        functools.partial(local, n, slabs),
        mesh=mesh,
        in_specs=(
            P(None, "slab", "patch", None),
            P(None, ("slab", "patch"), None, None),
            P(),
            P("slab", None),
        ),
        out_specs=(P(None, "slab", "patch", None), P(None, ("slab", "patch"), None, None)),
        check_vma=False,
    )
```
